32 devices in a mesh: dp: 4 (over y, x), mp: 8 (over z, core).
Axes of the slice: x: 2, y: 2, z: 4, core: 2. Of those that a mesh axis runs over, the one named last changes fastest.
Arguments:
- block_input: bfloat16 [2048, 8, 2048], P('mp', 'dp'), may hold values from -6 to 6
- segments: int32 [8, 2048], P('dp'), may hold values from 0 to 5, never falling along the last dimension, each value on 1 to 1024 neighbouring positions
- key_keep: int32 [8, 2048], P('dp'), may hold values 0 or 1
- ln1_gain: float32 [2048], replicated, may hold values from 0.5 to 1.5
- ln1_bias: float32 [2048], replicated, may hold values from -1 to 1
- w_query: bfloat16 [2048, 2048], P(None, 'mp'), may hold values from -0.125 to 0.125
- b_query: float32 [2048], P('mp'), may hold values from -2.5 to 2.5
- w_keyval: bfloat16 [2048, 256], replicated, may hold values from -0.125 to 0.125
- b_value: float32 [128], replicated, may hold values from -2.5 to 2.5
- w_out: bfloat16 [2048, 2048], P('mp'), may hold values from -1 to 1
- b_out: float32 [2048], replicated, may hold values from -1.5 to 1.5
- ln2_gain: float32 [2048], replicated, may hold values from 0.5 to 1.5
- ln2_bias: float32 [2048], replicated, may hold values from -1 to 1
- w_up: bfloat16 [2048, 8192], P(None, 'mp'), may hold values from -0.125 to 0.125
- b_up: float32 [8192], P('mp'), may hold values from -2.5 to 2.5
- w_down: bfloat16 [8192, 2048], P('mp'), may hold values from -0.0625 to 0.0625
- b_down: float32 [2048], replicated, may hold values from -1.5 to 1.5
- cotangent: bfloat16 [2048, 8, 2048], P('mp', 'dp'), may hold values from -6 to 6
Outputs:
- result: bfloat16 [2048, 8, 2048], P('mp', 'dp')
- grad_input: bfloat16 [2048, 8, 2048], P('mp', 'dp')
- grad_ln1_gain: float32 [2048], replicated
- grad_ln1_bias: float32 [2048], replicated
- grad_w_query: float32 [2048, 2048], P(None, 'mp')
- grad_b_query: float32 [2048], P('mp')
- grad_w_keyval: float32 [2048, 256], replicated
- grad_b_value: float32 [128], replicated
- grad_w_out: float32 [2048, 2048], P('mp')
- grad_b_out: float32 [2048], replicated
- grad_ln2_gain: float32 [2048], replicated
- grad_ln2_bias: float32 [2048], replicated
- grad_w_up: float32 [2048, 8192], P(None, 'mp')
- grad_b_up: float32 [8192], P('mp')
- grad_w_down: float32 [8192, 2048], P('mp')
- grad_b_down: float32 [2048], replicated
The draws below stay inside these ranges and needn't reach their ends.
Inputs may be any that keep to these rules, and one draw needn't show every extreme that they name: `segments`: along each row the document numbers never fall; each of the 6 documents of a row holds one to half of 2048 positions. `key_keep`: a position always attends itself whatever its mark.
All inputs are finite; a program needn't handle non-finite values. No bound on the sum of `key_keep` on one device may be relied on, other than what follows from the above.
Results may differ from the reference program's by a relative error of at most 0.017.
Values may be sent and summed in bfloat16 or wider, within the bound.
A program may use at most 320 MiB of HBM per device.

```python
import math
import jax
import jax.numpy as jnp
import numpy as np
from jax import lax

H = 16
HD = 128
D = 2048
FF = 8192
LEN = 2048
DOCS = 6
NROWS = 8


def set_ends(entries, stream_key, least, high):
    extent = entries.shape
    place = [jax.random.randint(jax.random.fold_in(stream_key, axis), (), 0, extent[axis]) for axis in range(len(extent))]
    entries = entries.at[tuple(place)].set(least)
    longest = extent.index(max(extent))
    place[longest] = (place[longest] + 1) % extent[longest]
    return entries.at[tuple(place)].set(high)


def block_scale(stream_key, shape, cuts, low, high):
    factor_of, own = 1.0, jax.random.fold_in(stream_key, 6)
    for dim, blocks in cuts:
        steps = jnp.exp(jax.random.uniform(jax.random.fold_in(own, dim), (blocks,), jnp.float32, low / len(cuts), high / len(cuts)))
        factor_of = factor_of * jnp.repeat(steps, shape[dim] // blocks).reshape([-1 if axis == dim else 1 for axis in range(len(shape))])
    return factor_of


def profile(count, total, bound, skew):
    weights = [(1 << 20) // math.isqrt(rank ** skew) + 1 for rank in range(2, count + 1)]
    rest, counts = total - bound - (count - 1), [1] * (count - 1)
    while rest > 0:
        free = [i for i in range(count - 1) if counts[i] < bound]
        pool, left = sum([weights[i] for i in free]), rest
        for i in free:
            extra = min(bound - counts[i], max(1, left * weights[i] // pool), rest)
            counts[i] = counts[i] + extra
            rest = rest - extra
    return np.array([bound] + counts)


def uneven(key, number_of, total, most, skew):
    if number_of == 2:
        one = jax.random.randint(key, (), max(1, total - most), min(most, total - 1) + 1)
        return jnp.stack([one, total - one])
    sizes = jnp.asarray(profile(number_of, total, most, skew), jnp.int32)
    couples = (number_of - 1) // 2
    giver, receiver = sizes[1:1 + 2 * couples:2], sizes[2:2 + 2 * couples:2]
    margin = jnp.minimum(giver - 1, most - receiver)
    shifted = jax.random.randint(jax.random.fold_in(key, 1), (couples,), 0, 1 << 20) % (margin + 1)
    sizes = sizes.at[1:1 + 2 * couples:2].set(giver - shifted).at[2:2 + 2 * couples:2].set(receiver + shifted)
    return sizes[jax.random.permutation(jax.random.fold_in(key, 2), number_of)]


def gaussian(stream_key, extent, width, limit, pieces=(), kind=jnp.bfloat16):
    array = jax.random.normal(stream_key, extent, jnp.float32) * width
    if len(pieces) > 0:
        array = block_scale(stream_key, extent, pieces, -0.22, 0.18) * array
    return jnp.clip(array, min=-limit, max=limit).astype(kind)


def setup_inputs(seed: int = 0) -> dict:
    seeds = jax.random.split(jax.random.key(seed), 19)
    return {
        "block_input": gaussian(seeds[0], (LEN, NROWS, D), 1.0, 6.0, ((0, 8), (1, 4))),
        "segments": jax.vmap(lambda own: jnp.searchsorted(jnp.cumsum(uneven(own, DOCS, LEN, LEN // 2, 2)), jnp.arange(LEN), side="right"))(jax.random.split(seeds[1], NROWS)).reshape((NROWS, LEN)).astype(jnp.int32),
        "key_keep": set_ends((jax.random.randint(seeds[2], (NROWS, LEN), 0, 8) < 7).astype(jnp.int32), jax.random.fold_in(seeds[2], 1), 0, 1),
        "ln1_gain": jnp.clip(1.0 + 0.1 * jax.random.normal(seeds[3], (D,), jnp.float32), 0.5, 1.5),
        "ln1_bias": gaussian(seeds[4], (D,), 0.2, 1.0, (), jnp.float32),
        "w_query": gaussian(seeds[5], (D, D), D ** -0.5, 0.125, ((1, 8),)),
        "b_query": gaussian(seeds[6], (D,), 0.5, 2.5, ((0, 8),), jnp.float32),
        "w_keyval": gaussian(seeds[7], (D, 2 * HD), D ** -0.5, 0.125),
        "b_value": gaussian(seeds[8], (HD,), 0.5, 2.5, (), jnp.float32),
        "w_out": gaussian(seeds[9], (D, D), (max(D // 64, 8)) ** -0.5, 1.0, ((0, 8),)),
        "b_out": gaussian(seeds[10], (D,), 0.3, 1.5, (), jnp.float32),
        "ln2_gain": jnp.clip(1.0 + 0.1 * jax.random.normal(seeds[11], (D,), jnp.float32), 0.5, 1.5),
        "ln2_bias": gaussian(seeds[12], (D,), 0.2, 1.0, (), jnp.float32),
        "w_up": gaussian(seeds[13], (D, FF), D ** -0.5, 0.125, ((1, 8),)),
        "b_up": gaussian(seeds[14], (FF,), 0.5, 2.5, ((0, 8),), jnp.float32),
        "w_down": gaussian(seeds[15], (FF, D), FF ** -0.5, 0.0625, ((0, 8),)),
        "b_down": gaussian(seeds[16], (D,), 0.3, 1.5, (), jnp.float32),
        "cotangent": gaussian(seeds[17], (LEN, NROWS, D), 1.0, 6.0, ((0, 8), (1, 4))),
    }


EPS = 1e-05
NEG = -1000000000.0

@jax.custom_vjp
def low(v):
    return lax.optimization_barrier(v.astype(jnp.bfloat16)).astype(jnp.float32)

@jax.custom_vjp
def low_back(v):
    return v

def low_keep(v):
    return (low(v), None)

def low_pass(kept, grad):
    return (grad,)

def back_keep(v):
    return (v, None)

def back_low(kept, grad):
    return (low(grad),)
low.defvjp(low_keep, low_pass)
low_back.defvjp(back_keep, back_low)

def layer_norm(values, norm_gain, norm_shift):
    average = lax.optimization_barrier(jnp.mean(values, axis=-1, keepdims=True))
    centred = values - average
    variance = lax.optimization_barrier(jnp.mean(centred * centred, axis=-1, keepdims=True))
    return centred * lax.rsqrt(variance + EPS) * norm_gain + norm_shift

def product(left, right):
    return jnp.dot(left, right, precision=lax.Precision.HIGHEST)

def attend(queries, keys_all, values_all, segment_row, keep_row):
    blocks = min(512, LEN)
    block_count = LEN // blocks
    positions = jnp.arange(LEN, dtype=jnp.int32)

    def one_block(element):
        query_block, segment_block, place_block = element
        scores = jnp.einsum('qhe,ke->hqk', query_block, keys_all, precision=lax.Precision.HIGHEST) * HD ** (-0.5)
        earlier = positions[None, :] <= place_block[:, None]
        same_doc = segment_row[None, :] == segment_block[:, None]
        open_key = (keep_row[None, :] == 1) | (positions[None, :] == place_block[:, None])
        allowed = earlier & same_doc & open_key
        scores = low_back(jnp.where(allowed[None], scores, NEG))
        weights = low(jax.nn.softmax(scores, axis=-1))
        return jnp.einsum('hqk,ke->qhe', weights, values_all, precision=lax.Precision.HIGHEST)
    outcome = lax.map(jax.checkpoint(one_block), (queries.reshape(block_count, blocks, H, HD), segment_row.reshape(block_count, blocks), positions.reshape(block_count, blocks)))
    return outcome.reshape(LEN, H * HD)

def forward(input_row, params, segment_row, keep_row):
    ln1_gain, ln1_bias, w_query, b_query, w_keyval, b_value, w_out, b_out, ln2_gain, ln2_bias, w_up, b_up, w_down, b_down = params
    normed = low(layer_norm(input_row, ln1_gain, ln1_bias))
    queries = low_back(low(product(normed, w_query) + b_query))
    projected = product(normed, w_keyval)
    keys_all = low_back(low(projected[:, :HD]))
    values_all = low_back(low(projected[:, HD:] + b_value))
    attended = low_back(low(attend(queries.reshape(LEN, H, HD), keys_all, values_all, segment_row, keep_row)))
    residual = input_row + low_back(product(attended, w_out)) + b_out
    normed_two = low(layer_norm(residual, ln2_gain, ln2_bias))
    pre_act = low_back(product(normed_two, w_up) + b_up)
    activated = low(jax.nn.gelu(pre_act, approximate=True))
    return residual + low_back(product(activated, w_down)) + b_down

def reference(block_input, segments, key_keep, ln1_gain, ln1_bias, w_query, b_query, w_keyval, b_value, w_out, b_out, ln2_gain, ln2_bias, w_up, b_up, w_down, b_down, cotangent):
    params = tuple((p.astype(jnp.float32) for p in (ln1_gain, ln1_bias, w_query, b_query, w_keyval, b_value, w_out, b_out, ln2_gain, ln2_bias, w_up, b_up, w_down, b_down)))

    def one_row(totals, element):
        input_row, segment_row, keep_row, grad_row = element

        def forward_row(input_value, *weights):
            return forward(input_value, weights, segment_row, keep_row)
        outcome, pullback = jax.vjp(forward_row, input_row.astype(jnp.float32), *params)
        grads = pullback(grad_row.astype(jnp.float32))
        new_totals = tuple((a + b for a, b in zip(totals, grads[1:])))
        return (new_totals, (outcome.astype(jnp.bfloat16), grads[0].astype(jnp.bfloat16)))
    zeros = tuple((jnp.zeros_like(p) for p in params))
    totals, (outcomes, grad_rows) = lax.scan(one_row, zeros, (jnp.swapaxes(block_input, 0, 1), segments, key_keep, jnp.swapaxes(cotangent, 0, 1)))
    return (jnp.swapaxes(outcomes, 0, 1), jnp.swapaxes(grad_rows, 0, 1), totals[0], totals[1], totals[2], totals[3], totals[4], totals[5], totals[6], totals[7], totals[8], totals[9], totals[10], totals[11], totals[12], totals[13])
```

```python
import functools
import math

import jax
import jax.numpy as jnp
from jax import lax
from jax.experimental import pallas as pl
from jax.experimental.pallas import tpu as pltpu
from jax.sharding import PartitionSpec as P

HD = 128
EPS = 1e-05
NEG = -1000000000.0
LOG2E = math.log2(math.e)
BF = jnp.bfloat16
F32 = jnp.float32
GROUP = 4


def layer_norm(values, norm_gain, norm_shift):
    average = jnp.mean(values, axis=-1, keepdims=True)
    centred = values - average
    variance = jnp.mean(centred * centred, axis=-1, keepdims=True)
    return centred * lax.rsqrt(variance + EPS) * norm_gain + norm_shift


def dot(left, right, dims=((1,), (0,))):
    return lax.dot_general(left, right, (dims, ((), ())), preferred_element_type=F32)


def forward_kernel(span, q_ref, kv_ref, bias_ref, o_ref, log_ref, vt, acc, top, total):
    row = pl.program_id(0)
    first, mine = span[row], span[pl.num_programs(0)]
    heads = q_ref.shape[1] // HD
    factor = HD ** (-0.5) * LOG2E

    @pl.loop(first, mine + 1)
    def _(j):
        vt[j] = kv_ref[j, 0, :, HD:].T

    for start in range(0, heads, GROUP):
        group = range(start, min(start + GROUP, heads))

        def block(j, initial):
            keys = kv_ref[j, 0, :, :HD]
            mask = bias_ref[j, 0].astype(F32)
            for g, head in enumerate(group):
                query = q_ref[:, head * HD : (head + 1) * HD]
                score = dot(keys, query, ((1,), (1,))) * factor + mask
                high = jnp.max(score, axis=0, keepdims=True)
                if not initial:
                    old = top[g]
                    high = jnp.maximum(high, old)
                    fade = jnp.exp2(old - high)
                part = jnp.exp2(score - high)
                size = jnp.sum(part, axis=0, keepdims=True)
                mixed = dot(vt[j], part.astype(BF))
                top[g] = high
                total[g] = size if initial else total[g] * fade + size
                acc[g] = mixed if initial else acc[g] * fade + mixed

        block(mine, True)

        @pl.loop(first, mine)
        def _(j):
            block(j, False)

        for g, head in enumerate(group):
            size = total[g]
            o_ref[:, head * HD : (head + 1) * HD] = (acc[g] / size).T.astype(BF)
            log_ref[0, head : head + 1, :] = top[g] + jnp.log2(size)


def attention_forward(span, queries, keyval, bias, rows):
    tokens, width = queries.shape
    length = tokens // rows
    blocks = keyval.shape[0]
    heads = width // HD
    return pl.pallas_call(
        forward_kernel,
        out_shape=(
            jax.ShapeDtypeStruct((tokens, width), BF),
            jax.ShapeDtypeStruct((rows, heads, length), F32),
        ),
        grid_spec=pltpu.PrefetchScalarGridSpec(
            num_scalar_prefetch=1,
            grid=(rows,),
            in_specs=[
                pl.BlockSpec((length, width), lambda r, s: (r, 0)),
                pl.BlockSpec((blocks, 1, length, 2 * HD), lambda r, s: (0, r, 0, 0)),
                pl.BlockSpec((blocks, 1, length, length), lambda r, s: (0, r, 0, 0)),
            ],
            out_specs=(
                pl.BlockSpec((length, width), lambda r, s: (r, 0)),
                pl.BlockSpec((1, heads, length), lambda r, s: (r, 0, 0)),
            ),
            scratch_shapes=[
                pltpu.VMEM((blocks, HD, length), BF),
                pltpu.VMEM((GROUP, HD, length), F32),
                pltpu.VMEM((GROUP, 1, length), F32),
                pltpu.VMEM((GROUP, 1, length), F32),
            ],
        ),
        compiler_params=pltpu.CompilerParams(vmem_limit_bytes=40 * 2**20),
        cost_estimate=pl.CostEstimate(
            flops=rows * heads * length * 4 * length * HD * 4,
            bytes_accessed=4 * tokens * width,
            transcendentals=rows * heads * length * 4 * length,
        ),
        name="attention_forward",
    )(span, queries, keyval, bias)


def backward_kernel(
    span, q_ref, do_ref, o_ref, kv_ref, bias_ref, log_ref, dq_ref, dkv_ref,
    kt, dk, dv, dqt, delta,
):
    row = pl.program_id(0)
    first, mine = span[row], span[pl.num_programs(0)]
    heads = q_ref.shape[1] // HD
    scale = HD ** (-0.5)
    factor = scale * LOG2E

    dkv_ref[...] = jnp.zeros_like(dkv_ref)

    @pl.loop(first, mine + 1)
    def _(j):
        kt[j] = kv_ref[j, 0, :, :HD].T
        dk[j] = jnp.zeros(dk.shape[1:], F32)
        dv[j] = jnp.zeros(dv.shape[1:], F32)

    for head in range(heads):
        cols = slice(head * HD, (head + 1) * HD)
        product = do_ref[:, cols].astype(F32) * o_ref[:, cols].astype(F32)
        delta[head] = jnp.sum(product.T, axis=0, keepdims=True)

    for start in range(0, heads, GROUP):
        group = range(start, min(start + GROUP, heads))

        def block(j, initial):
            keys = kv_ref[j, 0, :, :HD]
            values = kv_ref[j, 0, :, HD:]
            mask = bias_ref[j, 0].astype(F32)
            sum_k, sum_v = dk[j], dv[j]
            for g, head in enumerate(group):
                query = q_ref[:, head * HD : (head + 1) * HD]
                grad = do_ref[:, head * HD : (head + 1) * HD]
                score = dot(keys, query, ((1,), (1,))) * factor + mask
                prob = jnp.exp2(score - log_ref[0, head : head + 1, :])
                grad_prob = dot(values, grad, ((1,), (1,)))
                grad_score = (prob * (grad_prob - delta[head])).astype(BF)
                sum_v = sum_v + dot(prob.astype(BF), grad)
                sum_k = sum_k + dot(grad_score, query)
                part = dot(kt[j], grad_score)
                dqt[g] = part if initial else dqt[g] + part
            dk[j] = sum_k
            dv[j] = sum_v

        block(mine, True)

        @pl.loop(first, mine)
        def _(j):
            block(j, False)

        for g, head in enumerate(group):
            dq_ref[:, head * HD : (head + 1) * HD] = (dqt[g] * scale).T.astype(BF)

    @pl.loop(first, mine + 1)
    def _(j):
        dkv_ref[j, 0, :, :HD] = (dk[j] * scale).astype(BF)
        dkv_ref[j, 0, :, HD:] = dv[j].astype(BF)


def attention_backward(span, queries, grad_out, out, keyval, bias, logs, rows):
    tokens, width = queries.shape
    length = tokens // rows
    blocks = keyval.shape[0]
    heads = width // HD
    slab = pl.BlockSpec((length, width), lambda r, s: (r, 0))
    pairs = pl.BlockSpec((blocks, 1, length, 2 * HD), lambda r, s: (0, r, 0, 0))
    return pl.pallas_call(
        backward_kernel,
        out_shape=(
            jax.ShapeDtypeStruct((tokens, width), BF),
            jax.ShapeDtypeStruct(keyval.shape, BF),
        ),
        grid_spec=pltpu.PrefetchScalarGridSpec(
            num_scalar_prefetch=1,
            grid=(rows,),
            in_specs=[
                slab,
                slab,
                slab,
                pairs,
                pl.BlockSpec((blocks, 1, length, length), lambda r, s: (0, r, 0, 0)),
                pl.BlockSpec((1, heads, length), lambda r, s: (r, 0, 0)),
            ],
            out_specs=(slab, pairs),
            scratch_shapes=[
                pltpu.VMEM((blocks, HD, length), BF),
                pltpu.VMEM((blocks, length, HD), F32),
                pltpu.VMEM((blocks, length, HD), F32),
                pltpu.VMEM((GROUP, HD, length), F32),
                pltpu.VMEM((heads, 1, length), F32),
            ],
        ),
        compiler_params=pltpu.CompilerParams(vmem_limit_bytes=40 * 2**20),
        cost_estimate=pl.CostEstimate(
            flops=rows * heads * length * 4 * length * HD * 10,
            bytes_accessed=8 * tokens * width,
            transcendentals=rows * heads * length * 4 * length,
        ),
        name="attention_backward",
    )(span, queries, grad_out, out, keyval, bias, logs)


def swap(x, axis, count, bit):
    return lax.ppermute(x, axis, [(i, i ^ bit) for i in range(count)])


def low_bit(slot):
    return slot & -slot


def high_bit(slot):
    return 1 << (slot.bit_length() - 1)


def by_bits(count):
    return sorted(range(1, count), key=lambda slot: (bin(slot).count("1"), slot))


def gather_slots(x, axis, count):
    half = x.shape[0] // 2
    slots = {0: (x[:half], x[half:], x)}
    for slot in by_bits(count):
        high, low = high_bit(slot), low_bit(slot)
        if high == low:
            whole = swap(x, axis, count, high)
            slots[slot] = (whole[:half], whole[half:], whole)
        else:
            first = swap(slots[slot ^ high][0], axis, count, high)
            second = swap(slots[slot ^ low][1], axis, count, low)
            slots[slot] = (first, second, None)
    return [
        slots[slot][2] if slots[slot][2] is not None else jnp.concatenate(slots[slot][:2])
        for slot in range(count)
    ]


def scatter_slots(blocks, axis, count):
    half = blocks[0].shape[0] // 2
    parts = {slot: [blocks[slot][:half], blocks[slot][half:]] for slot in range(count)}
    whole = dict(enumerate(blocks))

    def add(slot, which, value):
        parts[slot][which] = (
            parts[slot][which].astype(F32) + value.astype(F32)
        ).astype(blocks[slot].dtype)
        whole[slot] = None

    for slot in reversed(by_bits(count)):
        high, low = high_bit(slot), low_bit(slot)
        if high == low:
            value = whole[slot] if whole[slot] is not None else jnp.concatenate(parts[slot])
            got = swap(value, axis, count, high)
            add(0, 0, got[:half])
            add(0, 1, got[half:])
        else:
            add(slot ^ high, 0, swap(parts[slot][0], axis, count, high))
            add(slot ^ low, 1, swap(parts[slot][1], axis, count, low))
    return jnp.concatenate(parts[0])


def by_owner(slots, own, count):
    shape = slots[0].shape
    whole = jnp.zeros((count,) + shape, slots[0].dtype)
    for slot, value in enumerate(slots):
        start = (own ^ slot,) + (0,) * len(shape)
        whole = lax.dynamic_update_slice(whole, value[None], start)
    return whole.reshape((count * shape[0],) + shape[1:])


def total_over(x, axis, count, own):
    size = x.shape[0] // count
    blocks = [lax.dynamic_slice_in_dim(x, (own ^ slot) * size, size, 0) for slot in range(count)]
    return by_owner(gather_slots(scatter_slots(blocks, axis, count), axis, count), own, count)


def solution(mesh):
    ndp, nmp = mesh.shape["dp"], mesh.shape["mp"]

    def gather_mp(x):
        return lax.all_gather(x, "mp", axis=0, tiled=True)

    def scatter_mp(x):
        return lax.psum_scatter(x, "mp", scatter_dimension=0, tiled=True)

    def body(
        block_input, segments, key_keep, ln1_gain, ln1_bias, w_query, b_query, w_keyval,
        b_value, w_out, b_out, ln2_gain, ln2_bias, w_up, b_up, w_down, b_down, cotangent,
    ):
        length, rows, width = block_input.shape
        tokens = length * rows
        hidden = w_up.shape[1]
        unit = hidden // ndp
        dp, mp = lax.axis_index("dp"), lax.axis_index("mp")

        def by_row(x):
            return jnp.swapaxes(x, 0, 1).reshape(tokens, width)

        def by_place(x):
            return jnp.swapaxes(x.reshape(rows, length, width), 0, 1)

        local = by_row(block_input)
        cot = by_row(cotangent)
        local_input = local.astype(F32)

        query_t = gather_mp(w_query.T)
        out_full = gather_mp(w_out)
        up_t = gather_mp(lax.dynamic_slice_in_dim(w_up, dp * unit, unit, 1).T)
        down = gather_mp(lax.dynamic_slice_in_dim(w_down, dp * unit, unit, 0))
        biases = lax.all_gather(
            jnp.concatenate([b_query, lax.dynamic_slice_in_dim(b_up, dp * unit, unit, 0)]),
            "mp", axis=0, tiled=False,
        )
        query_bias = biases[:, : b_query.shape[0]].reshape(-1)
        up_bias = biases[:, b_query.shape[0] :].reshape(-1)

        places = jnp.arange(nmp * length, dtype=jnp.int32)
        own_places = mp * length + jnp.arange(length, dtype=jnp.int32)
        own_segments = lax.dynamic_slice_in_dim(segments, mp * length, length, 1)
        same_place = places[None, :, None] == own_places[None, None, :]
        allowed = (
            (places[None, :, None] <= own_places[None, None, :])
            & (segments[:, :, None] == own_segments[:, None, :])
            & ((key_keep[:, :, None] == 1) | same_place)
        )
        bias = jnp.where(allowed, 0.0, NEG).astype(BF)
        bias = jnp.swapaxes(bias.reshape(rows, nmp, length, length), 0, 1)
        doc_start = jnp.sum((segments < own_segments[:, :1]).astype(jnp.int32), axis=1)
        span = jnp.concatenate([doc_start // length, mp[None].astype(jnp.int32)])

        normed = layer_norm(local_input, ln1_gain, ln1_bias).astype(BF)
        projected = dot(normed, w_keyval)
        keyval_local = jnp.concatenate(
            [projected[:, :HD], projected[:, HD:] + b_value], axis=1
        ).astype(BF)
        keyval = lax.all_gather(
            keyval_local.reshape(rows, length, 2 * HD), "mp", axis=0, tiled=False
        )
        queries = (dot(normed, query_t, ((1,), (1,))) + query_bias).astype(BF)
        attended, logs = attention_forward(span, queries, keyval, bias, rows)
        residual = local_input + dot(attended, out_full) + b_out
        normed_two = layer_norm(residual, ln2_gain, ln2_bias).astype(BF)

        cot_slots = gather_slots(cot, "dp", ndp)
        two_slots = gather_slots(normed_two, "dp", ndp)
        grown, grad_two, acts, pres = [], [], [], []
        for slot in range(ndp):
            pre_act = dot(two_slots[slot], up_t, ((1,), (1,))) + up_bias
            gelu_value, gelu_pull = jax.vjp(
                lambda inner: jax.nn.gelu(inner, approximate=True), pre_act
            )
            grad_act = dot(cot_slots[slot], down, ((1,), (1,)))
            acts.append(gelu_value.astype(BF))
            pres.append(gelu_pull(grad_act)[0].astype(BF))
        for slot in range(ndp):
            kind = F32 if slot == 0 else BF
            grown.append(dot(acts[slot], down).astype(kind))
            grad_two.append(dot(pres[slot], up_t).astype(kind))
        grad_normed_two = scatter_slots(grad_two, "dp", ndp)
        act_full, pre_full = jnp.concatenate(acts), jnp.concatenate(pres)
        cot_full, two_full = jnp.concatenate(cot_slots), jnp.concatenate(two_slots)
        grad_down = dot(act_full, cot_full, ((0,), (0,))).astype(BF)
        grad_up = dot(pre_full, two_full, ((0,), (0,))).astype(BF)
        grad_b_up = jnp.sum(pre_full, axis=0, dtype=F32)
        grown_sum = scatter_slots(grown, "dp", ndp)
        result = (residual + grown_sum + b_down).astype(BF)

        grad_down = by_owner(gather_slots(scatter_mp(grad_down), "dp", ndp), dp, ndp)
        grad_up = by_owner(gather_slots(scatter_mp(grad_up), "dp", ndp), dp, ndp)

        norm_two_value, norm_two_pull = jax.vjp(layer_norm, residual, ln2_gain, ln2_bias)
        grad_resid_part, grad_ln2_gain, grad_ln2_bias = norm_two_pull(grad_normed_two)
        grad_residual = cot.astype(F32) + grad_resid_part
        grad_b_out = jnp.sum(grad_residual, axis=0)
        grad_b_down = jnp.sum(cot, axis=0, dtype=F32)
        grad_mixed = grad_residual.astype(BF)
        grad_attended = dot(grad_mixed, out_full, ((1,), (1,))).astype(BF)
        grad_out = scatter_mp(dot(attended, grad_mixed, ((0,), (0,))).astype(BF))
        grad_out = total_over(grad_out, "dp", ndp, dp)
        grad_queries, grad_keyval = attention_backward(
            span, queries, grad_attended, attended, keyval, bias, logs, rows
        )
        grad_keyval = scatter_mp(grad_keyval).reshape(tokens, 2 * HD)
        grad_b_query = jnp.sum(grad_queries, axis=0, dtype=F32)
        grad_query = scatter_mp(dot(grad_queries, normed, ((0,), (0,))).astype(BF))
        grad_query = total_over(grad_query, "dp", ndp, dp)
        grad_normed = dot(grad_queries, query_t) + dot(grad_keyval, w_keyval, ((1,), (1,)))
        grad_w_keyval = dot(normed, grad_keyval, ((0,), (0,)))
        grad_b_value = jnp.sum(grad_keyval[:, HD:], axis=0, dtype=F32)
        norm_one_value, norm_one_pull = jax.vjp(layer_norm, local_input, ln1_gain, ln1_bias)
        grad_local, grad_ln1_gain, grad_ln1_bias = norm_one_pull(grad_normed)
        grad_input = (grad_residual + grad_local).astype(BF)

        units = jnp.zeros((nmp, ndp, unit), F32)
        units = lax.dynamic_update_slice(units, grad_b_up.reshape(nmp, 1, unit), (0, dp, 0))
        small = [
            grad_ln1_gain, grad_ln1_bias, grad_ln2_gain, grad_ln2_bias,
            grad_b_out, grad_b_down, grad_b_query, units.reshape(-1), grad_b_value,
        ]
        sizes = [value.shape[0] for value in small]
        sums, grad_w_keyval = lax.psum((jnp.concatenate(small), grad_w_keyval), ("dp", "mp"))
        pieces, place = [], 0
        for size in sizes:
            pieces.append(sums[place : place + size])
            place += size

        def own_part(value, size):
            return lax.dynamic_slice_in_dim(value, mp * size, size, 0)

        return (
            by_place(result),
            by_place(grad_input),
            pieces[0],
            pieces[1],
            grad_query.T.astype(F32),
            own_part(pieces[6], b_query.shape[0]),
            grad_w_keyval,
            pieces[8],
            grad_out.astype(F32),
            pieces[4],
            pieces[2],
            pieces[3],
            grad_up.T.astype(F32),
            own_part(pieces[7], hidden),
            grad_down.astype(F32),
            pieces[5],
        )

    return jax.shard_map(
        body,
        mesh=mesh,
        in_specs=(
            P("mp", "dp", None),
            P("dp", None),
            P("dp", None),
            P(),
            P(),
            P(None, "mp"),
            P("mp"),
            P(),
            P(),
            P("mp", None),
            P(),
            P(),
            P(),
            P(None, "mp"),
            P("mp"),
            P("mp", None),
            P(),
            P("mp", "dp", None),
        ),
        out_specs=(
            P("mp", "dp", None),
            P("mp", "dp", None),
            P(),
            P(),
            P(None, "mp"),
            P("mp"),
            P(),
            P(),
            P("mp", None),
            P(),
            P(),
            P(),
            P(None, "mp"),
            P("mp"),
            P("mp", None),
            P(),
        ),
        check_vma=False,
    )
```

```python
import functools
import math

import jax
import jax.numpy as jnp
from jax import lax
from jax.experimental import pallas as pl
from jax.experimental.pallas import tpu as pltpu
from jax.sharding import PartitionSpec as P

HD = 128
EPS = 1e-05
NEG = -1000000000.0
LOG2E = math.log2(math.e)
BF = jnp.bfloat16
F32 = jnp.float32
GROUP = 4


def layer_norm(values, norm_gain, norm_shift):
    average = jnp.mean(values, axis=-1, keepdims=True)
    centred = values - average
    variance = jnp.mean(centred * centred, axis=-1, keepdims=True)
    return centred * lax.rsqrt(variance + EPS) * norm_gain + norm_shift


def dot(left, right, dims=((1,), (0,))):
    return lax.dot_general(left, right, (dims, ((), ())), preferred_element_type=F32)


def forward_kernel(span, q_ref, kv_ref, bias_ref, o_ref, log_ref, vt, acc, top, total):
    row = pl.program_id(0)
    first, mine = span[row], kv_ref.shape[0] - 1
    heads = q_ref.shape[1] // HD
    factor = HD ** (-0.5) * LOG2E

    @pl.loop(first, mine + 1)
    def _(j):
        vt[j] = kv_ref[j, 0, :, HD:].T

    for start in range(0, heads, GROUP):
        group = range(start, min(start + GROUP, heads))

        def block(j, initial):
            keys = kv_ref[j, 0, :, :HD]
            mask = bias_ref[j, 0].astype(F32)
            for g, head in enumerate(group):
                query = q_ref[:, head * HD : (head + 1) * HD]
                score = dot(keys, query, ((1,), (1,))) * factor + mask
                high = jnp.max(score, axis=0, keepdims=True)
                if not initial:
                    old = top[g]
                    high = jnp.maximum(high, old)
                    fade = jnp.exp2(old - high)
                part = jnp.exp2(score - high)
                size = jnp.sum(part, axis=0, keepdims=True)
                mixed = dot(vt[j], part.astype(BF))
                top[g] = high
                total[g] = size if initial else total[g] * fade + size
                acc[g] = mixed if initial else acc[g] * fade + mixed

        block(mine, True)

        @pl.loop(first, mine)
        def _(j):
            block(j, False)

        for g, head in enumerate(group):
            size = total[g]
            o_ref[:, head * HD : (head + 1) * HD] = (acc[g] / size).T.astype(BF)
            log_ref[0, head : head + 1, :] = top[g] + jnp.log2(size)


def attention_forward(span, queries, keyval, bias, rows):
    tokens, width = queries.shape
    length = tokens // rows
    blocks = keyval.shape[0]
    heads = width // HD
    return pl.pallas_call(
        forward_kernel,
        out_shape=(
            jax.ShapeDtypeStruct((tokens, width), BF),
            jax.ShapeDtypeStruct((rows, heads, length), F32),
        ),
        grid_spec=pltpu.PrefetchScalarGridSpec(
            num_scalar_prefetch=1,
            grid=(rows,),
            in_specs=[
                pl.BlockSpec((length, width), lambda r, s: (r, 0)),
                pl.BlockSpec((blocks, 1, length, 2 * HD), lambda r, s: (0, r, 0, 0)),
                pl.BlockSpec((blocks, 1, length, length), lambda r, s: (0, r, 0, 0)),
            ],
            out_specs=(
                pl.BlockSpec((length, width), lambda r, s: (r, 0)),
                pl.BlockSpec((1, heads, length), lambda r, s: (r, 0, 0)),
            ),
            scratch_shapes=[
                pltpu.VMEM((blocks, HD, length), BF),
                pltpu.VMEM((GROUP, HD, length), F32),
                pltpu.VMEM((GROUP, 1, length), F32),
                pltpu.VMEM((GROUP, 1, length), F32),
            ],
        ),
        compiler_params=pltpu.CompilerParams(vmem_limit_bytes=40 * 2**20),
        cost_estimate=pl.CostEstimate(
            flops=rows * heads * length * 4 * length * HD * 4,
            bytes_accessed=4 * tokens * width,
            transcendentals=rows * heads * length * 4 * length,
        ),
        name="attention_forward",
    )(span, queries, keyval, bias)


def backward_kernel(
    span, q_ref, do_ref, o_ref, kv_ref, bias_ref, log_ref, dq_ref, dkv_ref,
    kt, dk, dv, dqt, delta,
):
    row = pl.program_id(0)
    first, mine = span[row], kv_ref.shape[0] - 1
    heads = q_ref.shape[1] // HD
    scale = HD ** (-0.5)
    factor = scale * LOG2E

    dkv_ref[...] = jnp.zeros_like(dkv_ref)

    @pl.loop(first, mine + 1)
    def _(j):
        kt[j] = kv_ref[j, 0, :, :HD].T
        dk[j] = jnp.zeros(dk.shape[1:], F32)
        dv[j] = jnp.zeros(dv.shape[1:], F32)

    for head in range(heads):
        cols = slice(head * HD, (head + 1) * HD)
        product = do_ref[:, cols].astype(F32) * o_ref[:, cols].astype(F32)
        delta[head] = jnp.sum(product.T, axis=0, keepdims=True)

    for start in range(0, heads, GROUP):
        group = range(start, min(start + GROUP, heads))

        def block(j, initial):
            keys = kv_ref[j, 0, :, :HD]
            values = kv_ref[j, 0, :, HD:]
            mask = bias_ref[j, 0].astype(F32)
            sum_k, sum_v = dk[j], dv[j]
            for g, head in enumerate(group):
                query = q_ref[:, head * HD : (head + 1) * HD]
                grad = do_ref[:, head * HD : (head + 1) * HD]
                score = dot(keys, query, ((1,), (1,))) * factor + mask
                prob = jnp.exp2(score - log_ref[0, head : head + 1, :])
                grad_prob = dot(values, grad, ((1,), (1,)))
                grad_score = (prob * (grad_prob - delta[head])).astype(BF)
                sum_v = sum_v + dot(prob.astype(BF), grad)
                sum_k = sum_k + dot(grad_score, query)
                part = dot(kt[j], grad_score)
                dqt[g] = part if initial else dqt[g] + part
            dk[j] = sum_k
            dv[j] = sum_v

        block(mine, True)

        @pl.loop(first, mine)
        def _(j):
            block(j, False)

        for g, head in enumerate(group):
            dq_ref[:, head * HD : (head + 1) * HD] = (dqt[g] * scale).T.astype(BF)

    @pl.loop(first, mine + 1)
    def _(j):
        dkv_ref[j, 0, :, :HD] = (dk[j] * scale).astype(BF)
        dkv_ref[j, 0, :, HD:] = dv[j].astype(BF)


def attention_backward(span, queries, grad_out, out, keyval, bias, logs, rows):
    tokens, width = queries.shape
    length = tokens // rows
    blocks = keyval.shape[0]
    heads = width // HD
    slab = pl.BlockSpec((length, width), lambda r, s: (r, 0))
    pairs = pl.BlockSpec((blocks, 1, length, 2 * HD), lambda r, s: (0, r, 0, 0))
    return pl.pallas_call(
        backward_kernel,
        out_shape=(
            jax.ShapeDtypeStruct((tokens, width), BF),
            jax.ShapeDtypeStruct(keyval.shape, BF),
        ),
        grid_spec=pltpu.PrefetchScalarGridSpec(
            num_scalar_prefetch=1,
            grid=(rows,),
            in_specs=[
                slab,
                slab,
                slab,
                pairs,
                pl.BlockSpec((blocks, 1, length, length), lambda r, s: (0, r, 0, 0)),
                pl.BlockSpec((1, heads, length), lambda r, s: (r, 0, 0)),
            ],
            out_specs=(slab, pairs),
            scratch_shapes=[
                pltpu.VMEM((blocks, HD, length), BF),
                pltpu.VMEM((blocks, length, HD), F32),
                pltpu.VMEM((blocks, length, HD), F32),
                pltpu.VMEM((GROUP, HD, length), F32),
                pltpu.VMEM((heads, 1, length), F32),
            ],
        ),
        compiler_params=pltpu.CompilerParams(vmem_limit_bytes=40 * 2**20),
        cost_estimate=pl.CostEstimate(
            flops=rows * heads * length * 4 * length * HD * 10,
            bytes_accessed=8 * tokens * width,
            transcendentals=rows * heads * length * 4 * length,
        ),
        name="attention_backward",
    )(span, queries, grad_out, out, keyval, bias, logs)


def swap(x, axis, count, bit):
    return lax.ppermute(x, axis, [(i, i ^ bit) for i in range(count)])


def shift(x, axis, count, by):
    pairs = [(i, i + by) for i in range(count) if 0 <= i + by < count]
    return lax.ppermute(x, axis, pairs)


def low_bit(slot):
    return slot & -slot


def high_bit(slot):
    return 1 << (slot.bit_length() - 1)


def by_bits(count):
    return sorted(range(1, count), key=lambda slot: (bin(slot).count("1"), slot))


def gather_slots(x, axis, count):
    near = gather_near(x, axis, count)
    return gather_far(x, near, axis, count)


def gather_near(x, axis, count):
    return [swap(x, axis, count, slot) for slot in by_bits(count) if low_bit(slot) == slot]


def gather_far(x, near, axis, count):
    half = x.shape[0] // 2
    slots, near = {0: (x[:half], x[half:], x)}, list(near)
    for slot in by_bits(count):
        high, low = high_bit(slot), low_bit(slot)
        if high == low:
            whole = near.pop(0)
            slots[slot] = (whole[:half], whole[half:], whole)
        else:
            first = swap(slots[slot ^ high][0], axis, count, high)
            second = swap(slots[slot ^ low][1], axis, count, low)
            slots[slot] = (first, second, jnp.concatenate([first, second]))
    return [slots[slot][2] for slot in range(count)]


def scatter_slots(blocks, axis, count, step=1):
    half = blocks[0].shape[0] // 2
    parts = {slot: [blocks[slot][:half], blocks[slot][half:]] for slot in range(len(blocks))}
    whole = dict(enumerate(blocks))

    def add(slot, which, value):
        parts[slot][which] = (
            parts[slot][which].astype(F32) + value.astype(F32)
        ).astype(blocks[slot].dtype)
        whole[slot] = None

    for slot in reversed(by_bits(len(blocks))):
        high, low = high_bit(slot), low_bit(slot)
        if high == low:
            value = whole[slot] if whole[slot] is not None else jnp.concatenate(parts[slot])
            got = swap(value, axis, count, high * step)
            add(0, 0, got[:half])
            add(0, 1, got[half:])
        else:
            add(slot ^ high, 0, swap(parts[slot][0], axis, count, high * step))
            add(slot ^ low, 1, swap(parts[slot][1], axis, count, low * step))
    return jnp.concatenate(parts[0])


def tie(*values):
    return lax.optimization_barrier(values)


def weave_kernel(where, *refs):
    count = len(refs) - 4
    parts, (out, held, into, back) = refs[:count], refs[count:]
    slots = count // 2
    arrivals = [pltpu.make_async_copy(parts[i], held.at[i], into.at[i]) for i in range(count)]
    for copy in arrivals:
        copy.start()
    leaving = []
    for i in range(count):
        arrivals[i].wait()
        core = where[1] ^ (i // slots)
        owner = where[0] ^ (i % slots)
        copy = pltpu.make_async_copy(held.at[i], out.at[:, core, owner], back.at[i])
        copy.start()
        leaving.append(copy)
    for copy in leaving:
        copy.wait()


def weave(parts, where, slots):
    chips, rows, width = parts[0].shape
    count = len(parts)
    return pl.pallas_call(
        weave_kernel,
        out_shape=jax.ShapeDtypeStruct((chips, 2, slots, rows, width), parts[0].dtype),
        grid_spec=pltpu.PrefetchScalarGridSpec(
            num_scalar_prefetch=1,
            grid=(1,),
            in_specs=[pl.BlockSpec(memory_space=pl.ANY)] * count,
            out_specs=pl.BlockSpec(memory_space=pl.ANY),
            scratch_shapes=[
                pltpu.VMEM((count, chips, rows, width), parts[0].dtype),
                pltpu.SemaphoreType.DMA((count,)),
                pltpu.SemaphoreType.DMA((count,)),
            ],
        ),
        compiler_params=pltpu.CompilerParams(vmem_limit_bytes=40 * 2**20),
        cost_estimate=pl.CostEstimate(
            flops=0, bytes_accessed=4 * count * chips * rows * width, transcendentals=0
        ),
        name="weave",
    )(where, *parts)


def settle_kernel(turned, count, where, *refs):
    parts, out, held = refs[:count], refs[count], refs[count + 1]
    rows = parts[0].shape[0]
    target = held if turned else out
    for slot in range(count):
        start = pl.multiple_of((where[0] ^ slot) * rows, rows)
        target[pl.ds(start, rows), :] = parts[slot][...].astype(F32)
    if turned:
        step = 256
        for place in range(0, held.shape[1], step):
            out[place : place + step, :] = held[:, place : place + step].T


def settle(parts, where, turned):
    rows, width = parts[0].shape
    count = len(parts)
    whole = (count * rows, width)
    return pl.pallas_call(
        functools.partial(settle_kernel, turned, count),
        out_shape=jax.ShapeDtypeStruct(whole[::-1] if turned else whole, F32),
        grid_spec=pltpu.PrefetchScalarGridSpec(
            num_scalar_prefetch=1,
            grid=(1,),
            in_specs=[pl.BlockSpec((rows, width), lambda i, w: (0, 0))] * count,
            out_specs=pl.BlockSpec(whole[::-1] if turned else whole, lambda i, w: (0, 0)),
            scratch_shapes=[pltpu.VMEM(whole if turned else (8, 128), F32)],
        ),
        compiler_params=pltpu.CompilerParams(vmem_limit_bytes=56 * 2**20),
        cost_estimate=pl.CostEstimate(
            flops=0, bytes_accessed=6 * count * rows * width, transcendentals=0
        ),
        name="settle",
    )(where, *parts)


def pair_kernel(flip, where, left, right, *refs):
    out = refs[-1]
    product = dot(left[...], right[...], ((0,), (0,)))
    if flip:
        out[0] = product.astype(BF)
        return
    product = (product + refs[0][0].astype(F32)).astype(BF)
    slots, _, rows, _ = out.shape
    for owner in range(slots):
        out[where[0] ^ owner, 0] = product[owner * rows : (owner + 1) * rows]


def pair_product(where, left, right, chips, slots, addend=None):
    tokens, columns = left.shape
    width = right.shape[1]
    rows = columns // (2 * chips)
    flip = addend is None
    if flip:
        shape = (chips, rows, width)
        spec = pl.BlockSpec((1, rows, width), lambda z, w: (z, 0, 0))
    else:
        shape = (slots, chips, rows // slots, width)
        spec = pl.BlockSpec((slots, 1, rows // slots, width), lambda z, w: (0, z, 0, 0))
    return pl.pallas_call(
        functools.partial(pair_kernel, flip),
        out_shape=jax.ShapeDtypeStruct(shape, BF),
        grid_spec=pltpu.PrefetchScalarGridSpec(
            num_scalar_prefetch=1,
            grid=(chips,),
            in_specs=[
                pl.BlockSpec(
                    (tokens, rows),
                    lambda z, w: (0, 2 * z + (1 - w[1] if flip else w[1])),
                ),
                pl.BlockSpec((tokens, width), lambda z, w: (0, 0)),
            ]
            + ([] if flip else [pl.BlockSpec((1, rows, width), lambda z, w: (z, 0, 0))]),
            out_specs=spec,
        ),
        compiler_params=pltpu.CompilerParams(vmem_limit_bytes=40 * 2**20),
        cost_estimate=pl.CostEstimate(
            flops=tokens * columns * width,
            bytes_accessed=2 * (tokens * (columns + width) + columns * width),
            transcendentals=0,
        ),
        name="pair_product",
    )(where, left, right, *([] if flip else [addend]))


def total_kernel(bits, one, two, one_out, two_out, acc, sent, got, full, out_sem, in_sem):
    barrier = pltpu.get_barrier_semaphore()
    places, partners = [], []
    for axis, bit in bits:
        mine = lax.axis_index(axis)
        place = (mine // bit) % 2
        places.append(place)
        partners.append({axis: mine + (1 - 2 * place) * bit})
    for partner in partners:
        pl.semaphore_signal(
            barrier, inc=1, device_id=partner, device_id_type=pl.DeviceIdType.MESH
        )
    split = one.shape[0]
    acc[:split, :] = one[...]
    acc[split:, :] = two[...]
    pl.semaphore_wait(barrier, len(bits))
    size, start, used = acc.shape[0], 0, 0
    starts = []
    for step in range(len(bits)):
        half, place = size // 2, places[step]
        keep = pl.multiple_of(start + place * half, 16)
        give = pl.multiple_of(start + (1 - place) * half, 16)
        region = pl.ds(used, half)
        sent[region, :] = acc[pl.ds(give, half), :].astype(BF)
        copy = pltpu.make_async_remote_copy(
            src_ref=sent.at[region],
            dst_ref=got.at[region],
            send_sem=out_sem.at[step],
            recv_sem=in_sem.at[step],
            device_id=partners[step],
            device_id_type=pl.DeviceIdType.MESH,
        )
        copy.start()
        copy.wait()
        acc[pl.ds(keep, half), :] = acc[pl.ds(keep, half), :] + got[region, :].astype(F32)
        starts.append(keep)
        start, size, used = keep, half, used + half
    full[pl.ds(start, size), :] = acc[pl.ds(start, size), :].astype(BF)
    for step in reversed(range(len(bits))):
        region = pl.ds(starts[step], size)
        copy = pltpu.make_async_remote_copy(
            src_ref=full.at[region],
            dst_ref=full.at[region],
            send_sem=out_sem.at[len(bits) + step],
            recv_sem=in_sem.at[len(bits) + step],
            device_id=partners[step],
            device_id_type=pl.DeviceIdType.MESH,
        )
        copy.start()
        copy.wait()
        size = 2 * size
    one_out[...] = full[:split, :].astype(F32)
    two_out[...] = full[split:, :].astype(F32)


def total(one, two, sizes):
    bits = []
    for axis, count in (("mp", 2), *sizes):
        bit = 1 if (axis, count) == ("mp", 2) and not bits else (2 if axis == "mp" else 1)
        while bit < count:
            bits.append((axis, bit))
            bit *= 2
    rows, width = one.shape[0] + two.shape[0], one.shape[1]
    return pl.pallas_call(
        functools.partial(total_kernel, tuple(bits)),
        out_shape=(
            jax.ShapeDtypeStruct(one.shape, F32),
            jax.ShapeDtypeStruct(two.shape, F32),
        ),
        in_specs=[pl.BlockSpec(memory_space=pltpu.VMEM)] * 2,
        out_specs=(pl.BlockSpec(memory_space=pltpu.VMEM),) * 2,
        scratch_shapes=[
            pltpu.VMEM((rows, width), F32),
            pltpu.VMEM((rows, width), BF),
            pltpu.VMEM((rows, width), BF),
            pltpu.VMEM((rows, width), BF),
            pltpu.SemaphoreType.DMA((2 * len(bits),)),
            pltpu.SemaphoreType.DMA((2 * len(bits),)),
        ],
        compiler_params=pltpu.CompilerParams(
            collective_id=0, has_side_effects=True, vmem_limit_bytes=40 * 2**20
        ),
        name="total",
    )(one, two)


def solution(mesh):
    ndp, nmp = mesh.shape["dp"], mesh.shape["mp"]

    def gather_mp(x):
        return lax.all_gather(x, "mp", axis=0, tiled=True)

    chips_of_core = [[core + 2 * chip for chip in range(nmp // 2)] for core in range(2)]

    def scatter_mp(x):
        return lax.psum_scatter(x, "mp", scatter_dimension=0, tiled=True)

    def body(
        block_input, segments, key_keep, ln1_gain, ln1_bias, w_query, b_query, w_keyval,
        b_value, w_out, b_out, ln2_gain, ln2_bias, w_up, b_up, w_down, b_down, cotangent,
    ):
        length, rows, width = block_input.shape
        tokens = length * rows
        hidden = w_up.shape[1]
        unit = hidden // ndp
        dp, mp = lax.axis_index("dp"), lax.axis_index("mp")

        def by_row(x):
            return jnp.swapaxes(x, 0, 1).reshape(tokens, width)

        def by_place(x):
            return jnp.swapaxes(x.reshape(rows, length, width), 0, 1)

        local = by_row(block_input)
        cot = by_row(cotangent)
        local_input = local.astype(F32)

        part = w_query.shape[1] // ndp
        chips = nmp // 2
        chip, core = mp // 2, mp % 2
        where = jnp.stack([dp, core]).astype(jnp.int32)
        full_length = segments.shape[1]
        reach = min(nmp - 1, -(-(full_length // 2 - 1) // length))

        normed = layer_norm(local_input, ln1_gain, ln1_bias).astype(BF)
        projected = dot(normed, w_keyval)
        keyval = jnp.concatenate(
            [projected[:, :HD], projected[:, HD:] + b_value], axis=1
        ).astype(BF).reshape(rows, length, 2 * HD)
        keyval = jnp.stack(
            [shift(keyval, "mp", nmp, by) for by in range(reach, 0, -1)] + [keyval]
        )

        def piece(shard, size):
            return lax.dynamic_slice_in_dim(shard, dp * size, size, 0)

        head_parts = lax.all_gather(
            jnp.stack([piece(w_query.T, part), piece(w_out, part)]),
            "mp", axis=0, tiled=False, axis_index_groups=chips_of_core,
        )
        up_t = gather_mp(piece(w_up.T, unit))
        down = gather_mp(piece(w_down, unit))
        biases = lax.all_gather(
            jnp.concatenate([b_query, piece(b_up, unit)]), "mp", axis=0, tiled=False
        )
        query_bias = biases[:, : b_query.shape[0]].reshape(-1)
        up_bias = biases[:, b_query.shape[0] :].reshape(-1)

        def gather_heads(column):
            slots = gather_slots(column.reshape(chips * part, width), "dp", ndp)
            return slots, [swap(slot, "mp", nmp, 1) for slot in slots]

        def weave_heads(near, far):
            slots = [slot.reshape(chips, part, width) for slot in near + far]
            return weave(slots, where, ndp).reshape(nmp * ndp * part, width)

        def sum_heads(left, right):
            theirs = pair_product(where, left, right, chips, ndp)
            theirs = swap(theirs, "mp", nmp, 1)
            both = pair_product(where, left, right, chips, ndp, theirs)
            column = scatter_slots(
                [both[slot].reshape(chips * part, width) for slot in range(ndp)], "dp", ndp
            ).reshape(chips, part, width)
            blocks = [
                lax.dynamic_index_in_dim(column, chip ^ slot, 0, keepdims=False)
                for slot in range(chips)
            ]
            return gather_slots(scatter_slots(blocks, "mp", nmp, 2), "dp", ndp)

        cot_near = gather_near(cot, "dp", ndp)
        head_parts, *cot_near = tie(head_parts, *cot_near)
        near, far = gather_heads(head_parts[:, 0])
        *cot_near, out_column = tie(*cot_near, head_parts[:, 1], *near)[: ndp.bit_length()]
        query_t = weave_heads(near, far)
        out_near, out_far = gather_heads(out_column)
        cot_slots = gather_far(cot, cot_near, "dp", ndp)

        window = (reach + 1) * length
        places = (mp - reach) * length + jnp.arange(window, dtype=jnp.int32)
        own_places = mp * length + jnp.arange(length, dtype=jnp.int32)

        def of_window(values):
            padded = jnp.pad(values, ((0, 0), (reach * length, 0)), constant_values=-1)
            return lax.dynamic_slice_in_dim(padded, mp * length, window, 1)

        own_segments = lax.dynamic_slice_in_dim(segments, mp * length, length, 1)
        same_place = places[None, :, None] == own_places[None, None, :]
        allowed = (
            (places[None, :, None] <= own_places[None, None, :])
            & (of_window(segments)[:, :, None] == own_segments[:, None, :])
            & ((of_window(key_keep)[:, :, None] == 1) | same_place)
        )
        bias = jnp.where(allowed, 0.0, NEG).astype(BF)
        bias = jnp.swapaxes(bias.reshape(rows, reach + 1, length, length), 0, 1)
        doc_start = jnp.sum((segments < own_segments[:, :1]).astype(jnp.int32), axis=1)
        span = jnp.maximum(doc_start // length - mp + reach, 0).astype(jnp.int32)

        queries = (dot(normed, query_t, ((1,), (1,))) + query_bias).astype(BF)
        attended, logs = attention_forward(span, queries, keyval, bias, rows)
        attended, *cot_slots = tie(attended, *cot_slots)
        out_full = weave_heads(out_near, out_far)
        residual = local_input + dot(attended, out_full) + b_out
        normed_two = layer_norm(residual, ln2_gain, ln2_bias).astype(BF)

        two_slots = gather_slots(normed_two, "dp", ndp)
        grown, grad_two, acts, slopes, pres = [], [], [], [], []
        for slot in range(ndp):
            pre_act = dot(two_slots[slot], up_t, ((1,), (1,))) + up_bias
            gelu_value, gelu_pull = jax.vjp(
                lambda inner: jax.nn.gelu(inner, approximate=True), pre_act
            )
            acts.append(gelu_value.astype(BF))
            slopes.append(gelu_pull(jnp.ones_like(pre_act))[0].astype(BF))
        act_full, cot_full = jnp.concatenate(acts), jnp.concatenate(cot_slots)
        grad_down = dot(act_full, cot_full, ((0,), (0,))).astype(BF)
        down, grad_down = tie(down, grad_down)
        grad_down = scatter_mp(grad_down)
        for slot in range(ndp):
            grad_act = dot(cot_slots[slot], down, ((1,), (1,)))
            pres.append((grad_act * slopes[slot].astype(F32)).astype(BF))
        for slot in reversed(range(ndp)):
            grad_two.append(dot(pres[slot], up_t).astype(F32 if slot == 0 else BF))
            if 0 < slot:
                pres[slot - 1], grad_two[-1] = tie(pres[slot - 1], grad_two[-1])
        grad_normed_two = scatter_slots(grad_two[::-1], "dp", ndp)
        two_full, pre_full = jnp.concatenate(two_slots), jnp.concatenate(pres)
        grad_up = dot(pre_full, two_full, ((0,), (0,))).astype(BF)
        grad_b_up = jnp.sum(pre_full, axis=0, dtype=F32)
        for slot in reversed(range(ndp)):
            grown.append(dot(acts[slot], down).astype(F32 if slot == 0 else BF))
        grad_normed_two, grad_up, *grown = tie(grad_normed_two, grad_up, *grown)
        grown_sum = scatter_slots(grown[::-1], "dp", ndp)
        result = (residual + grown_sum + b_down).astype(BF)
        grad_up = scatter_mp(grad_up)

        norm_two_value, norm_two_pull = jax.vjp(layer_norm, residual, ln2_gain, ln2_bias)
        grad_resid_part, grad_ln2_gain, grad_ln2_bias = norm_two_pull(grad_normed_two)
        grad_residual = cot.astype(F32) + grad_resid_part
        grad_b_out = jnp.sum(grad_residual, axis=0)
        grad_b_down = jnp.sum(cot, axis=0, dtype=F32)
        grad_mixed = grad_residual.astype(BF)
        grad_attended = dot(grad_mixed, out_full, ((1,), (1,))).astype(BF)
        grad_attended, grad_down = tie(grad_attended, grad_down)
        down_slots = gather_slots(grad_down, "dp", ndp)
        out_slots = sum_heads(attended, grad_mixed)
        grad_queries, grad_keyval = attention_backward(
            span, queries, grad_attended, attended, keyval, bias, logs, rows
        )
        grad_keyval = sum(
            (
                shift(grad_keyval[reach - by], "mp", nmp, -by).astype(F32)
                for by in range(1, reach + 1)
            ),
            grad_keyval[reach].astype(F32),
        ).astype(BF).reshape(tokens, 2 * HD)
        grad_b_query = jnp.sum(grad_queries, axis=0, dtype=F32)
        query_slots = sum_heads(grad_queries, normed)
        grad_keyval, grad_up = tie(grad_keyval, grad_up)
        up_slots = gather_slots(grad_up, "dp", ndp)
        grad_normed = dot(grad_queries, query_t) + dot(grad_keyval, w_keyval, ((1,), (1,)))
        grad_w_keyval = dot(normed, grad_keyval, ((0,), (0,)))
        grad_b_value = jnp.sum(grad_keyval[:, HD:], axis=0, dtype=F32)
        norm_one_value, norm_one_pull = jax.vjp(layer_norm, local_input, ln1_gain, ln1_bias)
        grad_local, grad_ln1_gain, grad_ln1_bias = norm_one_pull(grad_normed)
        grad_input = (grad_residual + grad_local).astype(BF)

        units = jnp.zeros((nmp, ndp, unit), F32)
        units = lax.dynamic_update_slice(units, grad_b_up.reshape(nmp, 1, unit), (0, dp, 0))
        small = [
            grad_ln1_gain, grad_ln1_bias, grad_ln2_gain, grad_ln2_bias,
            grad_b_out, grad_b_down, grad_b_query, units.reshape(-1), grad_b_value,
        ]
        sizes = [value.shape[0] for value in small]
        cells = sum(sizes)
        lines = -(-cells // (2 * HD))
        lines += -(lines + width) % (16 * ndp * nmp)
        small.append(jnp.zeros((lines * 2 * HD - cells,), F32))
        small = jnp.concatenate(small).reshape(lines, 2 * HD)
        grad_w_keyval, sums = total(
            grad_w_keyval, small, (("dp", ndp), ("mp", nmp))
        )
        sums = sums.reshape(-1)
        pieces, place = [], 0
        for size in sizes:
            pieces.append(sums[place : place + size])
            place += size

        def own_part(value, size):
            return lax.dynamic_slice_in_dim(value, mp * size, size, 0)

        return (
            by_place(result),
            by_place(grad_input),
            pieces[0],
            pieces[1],
            settle(query_slots, where, True),
            own_part(pieces[6], b_query.shape[0]),
            grad_w_keyval,
            pieces[8],
            settle(out_slots, where, False),
            pieces[4],
            pieces[2],
            pieces[3],
            settle(up_slots, where, True),
            own_part(pieces[7], hidden),
            settle(down_slots, where, False),
            pieces[5],
        )

    return jax.shard_map(
        body,
        mesh=mesh,
        in_specs=(
            P("mp", "dp", None),
            P("dp", None),
            P("dp", None),
            P(),
            P(),
            P(None, "mp"),
            P("mp"),
            P(),
            P(),
            P("mp", None),
            P(),
            P(),
            P(),
            P(None, "mp"),
            P("mp"),
            P("mp", None),
            P(),
            P("mp", "dp", None),
        ),
        out_specs=(
            P("mp", "dp", None),
            P("mp", "dp", None),
            P(),
            P(),
            P(None, "mp"),
            P("mp"),
            P(),
            P(),
            P("mp", None),
            P(),
            P(),
            P(),
            P(None, "mp"),
            P("mp"),
            P("mp", None),
            P(),
        ),
        check_vma=False,
    )
```

```python
import functools
import math

import jax
import jax.numpy as jnp
from jax import lax
from jax.experimental import pallas as pl
from jax.experimental.pallas import tpu as pltpu
from jax.sharding import PartitionSpec as P

HD = 128
EPS = 1e-05
NEG = -1000000000.0
LOG2E = math.log2(math.e)
BF = jnp.bfloat16
F32 = jnp.float32
GROUP = 4


def layer_norm(values, norm_gain, norm_shift):
    average = jnp.mean(values, axis=-1, keepdims=True)
    centred = values - average
    variance = jnp.mean(centred * centred, axis=-1, keepdims=True)
    return centred * lax.rsqrt(variance + EPS) * norm_gain + norm_shift


def dot(left, right, dims=((1,), (0,))):
    return lax.dot_general(left, right, (dims, ((), ())), preferred_element_type=F32)


def forward_kernel(span, q_ref, kv_ref, bias_ref, o_ref, log_ref, vt, acc, top, total):
    row = pl.program_id(0)
    first, mine = span[row], kv_ref.shape[0] - 1
    heads = q_ref.shape[1] // HD
    factor = HD ** (-0.5) * LOG2E

    @pl.loop(first, mine + 1)
    def _(j):
        vt[j] = kv_ref[j, 0, :, HD:].T

    for start in range(0, heads, GROUP):
        group = range(start, min(start + GROUP, heads))

        def block(j, initial):
            keys = kv_ref[j, 0, :, :HD]
            mask = bias_ref[j, 0].astype(F32)
            for g, head in enumerate(group):
                query = q_ref[:, head * HD : (head + 1) * HD]
                score = dot(keys, query, ((1,), (1,))) * factor + mask
                high = jnp.max(score, axis=0, keepdims=True)
                if not initial:
                    old = top[g]
                    high = jnp.maximum(high, old)
                    fade = jnp.exp2(old - high)
                part = jnp.exp2(score - high)
                size = jnp.sum(part, axis=0, keepdims=True)
                mixed = dot(vt[j], part.astype(BF))
                top[g] = high
                total[g] = size if initial else total[g] * fade + size
                acc[g] = mixed if initial else acc[g] * fade + mixed

        block(mine, True)

        @pl.loop(first, mine)
        def _(j):
            block(j, False)

        for g, head in enumerate(group):
            size = total[g]
            o_ref[:, head * HD : (head + 1) * HD] = (acc[g] / size).T.astype(BF)
            log_ref[0, head : head + 1, :] = top[g] + jnp.log2(size)


def attention_forward(span, queries, keyval, bias, rows):
    tokens, width = queries.shape
    length = tokens // rows
    blocks = keyval.shape[0]
    heads = width // HD
    return pl.pallas_call(
        forward_kernel,
        out_shape=(
            jax.ShapeDtypeStruct((tokens, width), BF),
            jax.ShapeDtypeStruct((rows, heads, length), F32),
        ),
        grid_spec=pltpu.PrefetchScalarGridSpec(
            num_scalar_prefetch=1,
            grid=(rows,),
            in_specs=[
                pl.BlockSpec((length, width), lambda r, s: (r, 0)),
                pl.BlockSpec((blocks, 1, length, 2 * HD), lambda r, s: (0, r, 0, 0)),
                pl.BlockSpec((blocks, 1, length, length), lambda r, s: (0, r, 0, 0)),
            ],
            out_specs=(
                pl.BlockSpec((length, width), lambda r, s: (r, 0)),
                pl.BlockSpec((1, heads, length), lambda r, s: (r, 0, 0)),
            ),
            scratch_shapes=[
                pltpu.VMEM((blocks, HD, length), BF),
                pltpu.VMEM((GROUP, HD, length), F32),
                pltpu.VMEM((GROUP, 1, length), F32),
                pltpu.VMEM((GROUP, 1, length), F32),
            ],
        ),
        compiler_params=pltpu.CompilerParams(vmem_limit_bytes=40 * 2**20),
        cost_estimate=pl.CostEstimate(
            flops=rows * heads * length * 4 * length * HD * 4,
            bytes_accessed=4 * tokens * width,
            transcendentals=rows * heads * length * 4 * length,
        ),
        name="attention_forward",
    )(span, queries, keyval, bias)


def backward_kernel(
    span, q_ref, do_ref, o_ref, kv_ref, bias_ref, log_ref, dq_ref, dkv_ref,
    kt, dk, dv, dqt, delta,
):
    row = pl.program_id(0)
    first, mine = span[row], kv_ref.shape[0] - 1
    heads = q_ref.shape[1] // HD
    scale = HD ** (-0.5)
    factor = scale * LOG2E

    dkv_ref[...] = jnp.zeros_like(dkv_ref)

    @pl.loop(first, mine + 1)
    def _(j):
        kt[j] = kv_ref[j, 0, :, :HD].T
        dk[j] = jnp.zeros(dk.shape[1:], F32)
        dv[j] = jnp.zeros(dv.shape[1:], F32)

    for head in range(heads):
        cols = slice(head * HD, (head + 1) * HD)
        product = do_ref[:, cols].astype(F32) * o_ref[:, cols].astype(F32)
        delta[head] = jnp.sum(product.T, axis=0, keepdims=True)

    for start in range(0, heads, GROUP):
        group = range(start, min(start + GROUP, heads))

        def block(j, initial):
            keys = kv_ref[j, 0, :, :HD]
            values = kv_ref[j, 0, :, HD:]
            mask = bias_ref[j, 0].astype(F32)
            sum_k, sum_v = dk[j], dv[j]
            for g, head in enumerate(group):
                query = q_ref[:, head * HD : (head + 1) * HD]
                grad = do_ref[:, head * HD : (head + 1) * HD]
                score = dot(keys, query, ((1,), (1,))) * factor + mask
                prob = jnp.exp2(score - log_ref[0, head : head + 1, :])
                grad_prob = dot(values, grad, ((1,), (1,)))
                grad_score = (prob * (grad_prob - delta[head])).astype(BF)
                sum_v = sum_v + dot(prob.astype(BF), grad)
                sum_k = sum_k + dot(grad_score, query)
                part = dot(kt[j], grad_score)
                dqt[g] = part if initial else dqt[g] + part
            dk[j] = sum_k
            dv[j] = sum_v

        block(mine, True)

        @pl.loop(first, mine)
        def _(j):
            block(j, False)

        for g, head in enumerate(group):
            dq_ref[:, head * HD : (head + 1) * HD] = (dqt[g] * scale).T.astype(BF)

    @pl.loop(first, mine + 1)
    def _(j):
        dkv_ref[j, 0, :, :HD] = (dk[j] * scale).astype(BF)
        dkv_ref[j, 0, :, HD:] = dv[j].astype(BF)


def attention_backward(span, queries, grad_out, out, keyval, bias, logs, rows):
    tokens, width = queries.shape
    length = tokens // rows
    blocks = keyval.shape[0]
    heads = width // HD
    slab = pl.BlockSpec((length, width), lambda r, s: (r, 0))
    pairs = pl.BlockSpec((blocks, 1, length, 2 * HD), lambda r, s: (0, r, 0, 0))
    return pl.pallas_call(
        backward_kernel,
        out_shape=(
            jax.ShapeDtypeStruct((tokens, width), BF),
            jax.ShapeDtypeStruct(keyval.shape, BF),
        ),
        grid_spec=pltpu.PrefetchScalarGridSpec(
            num_scalar_prefetch=1,
            grid=(rows,),
            in_specs=[
                slab,
                slab,
                slab,
                pairs,
                pl.BlockSpec((blocks, 1, length, length), lambda r, s: (0, r, 0, 0)),
                pl.BlockSpec((1, heads, length), lambda r, s: (r, 0, 0)),
            ],
            out_specs=(slab, pairs),
            scratch_shapes=[
                pltpu.VMEM((blocks, HD, length), BF),
                pltpu.VMEM((blocks, length, HD), F32),
                pltpu.VMEM((blocks, length, HD), F32),
                pltpu.VMEM((GROUP, HD, length), F32),
                pltpu.VMEM((heads, 1, length), F32),
            ],
        ),
        compiler_params=pltpu.CompilerParams(vmem_limit_bytes=40 * 2**20),
        cost_estimate=pl.CostEstimate(
            flops=rows * heads * length * 4 * length * HD * 10,
            bytes_accessed=8 * tokens * width,
            transcendentals=rows * heads * length * 4 * length,
        ),
        name="attention_backward",
    )(span, queries, grad_out, out, keyval, bias, logs)


def swap(x, axis, count, bit):
    return lax.ppermute(x, axis, [(i, i ^ bit) for i in range(count)])


def shift(x, axis, count, by):
    pairs = [(i, i + by) for i in range(count) if 0 <= i + by < count]
    return lax.ppermute(x, axis, pairs)


def low_bit(slot):
    return slot & -slot


def high_bit(slot):
    return 1 << (slot.bit_length() - 1)


def by_bits(count):
    return sorted(range(1, count), key=lambda slot: (bin(slot).count("1"), slot))


def gather_slots(x, axis, count):
    near = gather_near(x, axis, count)
    return gather_far(x, near, axis, count)


def gather_near(x, axis, count):
    return [swap(x, axis, count, slot) for slot in by_bits(count) if low_bit(slot) == slot]


def gather_far(x, near, axis, count):
    half = x.shape[0] // 2
    slots, near = {0: (x[:half], x[half:], x)}, list(near)
    for slot in by_bits(count):
        high, low = high_bit(slot), low_bit(slot)
        if high == low:
            whole = near.pop(0)
            slots[slot] = (whole[:half], whole[half:], whole)
        else:
            first = swap(slots[slot ^ high][0], axis, count, high)
            second = swap(slots[slot ^ low][1], axis, count, low)
            slots[slot] = (first, second, jnp.concatenate([first, second]))
    return [slots[slot][2] for slot in range(count)]


def scatter_slots(blocks, axis, count, step=1):
    steps = scatter_steps(blocks, axis, count, step)
    try:
        values = next(steps)[1]
        while True:
            values = steps.send(values)[1]
    except StopIteration as end:
        return end.value


def scatter_steps(blocks, axis, count, step=1):
    half = blocks[0].shape[0] // 2
    parts = {slot: [blocks[slot][:half], blocks[slot][half:]] for slot in range(len(blocks))}
    whole = dict(enumerate(blocks))
    weight = lambda slot: bin(slot).count("1")

    def add(slot, which, value):
        parts[slot][which] = (
            parts[slot][which].astype(F32) + value.astype(F32)
        ).astype(blocks[slot].dtype)
        whole[slot] = None

    for level in range(weight(len(blocks) - 1), 0, -1):
        targets, values, places = [], [], []
        for slot in [slot for slot in by_bits(len(blocks)) if weight(slot) == level]:
            high, low = high_bit(slot), low_bit(slot)
            if high == low:
                targets.append(None)
                places.append(high)
                values.append(
                    whole[slot] if whole[slot] is not None else jnp.concatenate(parts[slot])
                )
            else:
                targets += [(slot ^ high, 0), (slot ^ low, 1)]
                places += [high, low]
                values += parts[slot]
        values = yield ("send", values)
        values = [swap(value, axis, count, bit * step) for value, bit in zip(values, places)]
        values = yield ("took", values)
        for target, value in zip(targets, values):
            if target is None:
                add(0, 0, value[:half])
                add(0, 1, value[half:])
            else:
                add(*target, value)
    return jnp.concatenate(parts[0])


def tie(*values):
    return lax.optimization_barrier(values)


def weave_kernel(where, *refs):
    count = len(refs) - 4
    parts, (out, held, into, back) = refs[:count], refs[count:]
    slots = count // 2
    arrivals = [pltpu.make_async_copy(parts[i], held.at[i], into.at[i]) for i in range(count)]
    for copy in arrivals:
        copy.start()
    leaving = []
    for i in range(count):
        arrivals[i].wait()
        core = where[1] ^ (i // slots)
        owner = where[0] ^ (i % slots)
        copy = pltpu.make_async_copy(held.at[i], out.at[:, core, owner], back.at[i])
        copy.start()
        leaving.append(copy)
    for copy in leaving:
        copy.wait()


def weave(parts, where, slots):
    chips, rows, width = parts[0].shape
    count = len(parts)
    return pl.pallas_call(
        weave_kernel,
        out_shape=jax.ShapeDtypeStruct((chips, 2, slots, rows, width), parts[0].dtype),
        grid_spec=pltpu.PrefetchScalarGridSpec(
            num_scalar_prefetch=1,
            grid=(1,),
            in_specs=[pl.BlockSpec(memory_space=pl.ANY)] * count,
            out_specs=pl.BlockSpec(memory_space=pl.ANY),
            scratch_shapes=[
                pltpu.VMEM((count, chips, rows, width), parts[0].dtype),
                pltpu.SemaphoreType.DMA((count,)),
                pltpu.SemaphoreType.DMA((count,)),
            ],
        ),
        compiler_params=pltpu.CompilerParams(vmem_limit_bytes=40 * 2**20),
        cost_estimate=pl.CostEstimate(
            flops=0, bytes_accessed=4 * count * chips * rows * width, transcendentals=0
        ),
        name="weave",
    )(where, *parts)


def settle_kernel(turned, count, where, *refs):
    parts, out, held = refs[:count], refs[count], refs[count + 1]
    rows = parts[0].shape[0]
    target = held if turned else out
    for slot in range(count):
        start = pl.multiple_of((where[0] ^ slot) * rows, rows)
        target[pl.ds(start, rows), :] = parts[slot][...].astype(F32)
    if turned:
        step = 256
        for place in range(0, held.shape[1], step):
            out[place : place + step, :] = held[:, place : place + step].T


def settle(parts, where, turned):
    rows, width = parts[0].shape
    count = len(parts)
    whole = (count * rows, width)
    return pl.pallas_call(
        functools.partial(settle_kernel, turned, count),
        out_shape=jax.ShapeDtypeStruct(whole[::-1] if turned else whole, F32),
        grid_spec=pltpu.PrefetchScalarGridSpec(
            num_scalar_prefetch=1,
            grid=(1,),
            in_specs=[pl.BlockSpec((rows, width), lambda i, w: (0, 0))] * count,
            out_specs=pl.BlockSpec(whole[::-1] if turned else whole, lambda i, w: (0, 0)),
            scratch_shapes=[pltpu.VMEM(whole if turned else (8, 128), F32)],
        ),
        compiler_params=pltpu.CompilerParams(vmem_limit_bytes=56 * 2**20),
        cost_estimate=pl.CostEstimate(
            flops=0, bytes_accessed=6 * count * rows * width, transcendentals=0
        ),
        name="settle",
    )(where, *parts)


def pair_kernel(flip, where, left, right, *refs):
    out = refs[-1]
    product = dot(left[...], right[...], ((0,), (0,)))
    if flip:
        out[0] = product.astype(BF)
        return
    product = (product + refs[0][0].astype(F32)).astype(BF)
    slots, _, rows, _ = out.shape
    for owner in range(slots):
        out[where[0] ^ owner, 0] = product[owner * rows : (owner + 1) * rows]


def pair_product(where, left, right, chips, slots, addend=None):
    tokens, columns = left.shape
    width = right.shape[1]
    rows = columns // (2 * chips)
    flip = addend is None
    if flip:
        shape = (chips, rows, width)
        spec = pl.BlockSpec((1, rows, width), lambda z, w: (z, 0, 0))
    else:
        shape = (slots, chips, rows // slots, width)
        spec = pl.BlockSpec((slots, 1, rows // slots, width), lambda z, w: (0, z, 0, 0))
    return pl.pallas_call(
        functools.partial(pair_kernel, flip),
        out_shape=jax.ShapeDtypeStruct(shape, BF),
        grid_spec=pltpu.PrefetchScalarGridSpec(
            num_scalar_prefetch=1,
            grid=(chips,),
            in_specs=[
                pl.BlockSpec(
                    (tokens, rows),
                    lambda z, w: (0, 2 * z + (1 - w[1] if flip else w[1])),
                ),
                pl.BlockSpec((tokens, width), lambda z, w: (0, 0)),
            ]
            + ([] if flip else [pl.BlockSpec((1, rows, width), lambda z, w: (z, 0, 0))]),
            out_specs=spec,
        ),
        compiler_params=pltpu.CompilerParams(vmem_limit_bytes=40 * 2**20),
        cost_estimate=pl.CostEstimate(
            flops=tokens * columns * width,
            bytes_accessed=2 * (tokens * (columns + width) + columns * width),
            transcendentals=0,
        ),
        name="pair_product",
    )(where, left, right, *([] if flip else [addend]))


def total_kernel(bits, one, two, one_out, two_out, acc, sent, got, full, out_sem, in_sem):
    barrier = pltpu.get_barrier_semaphore()
    places, partners = [], []
    for axis, bit in bits:
        mine = lax.axis_index(axis)
        place = (mine // bit) % 2
        places.append(place)
        partners.append({axis: mine + (1 - 2 * place) * bit})
    for partner in partners:
        pl.semaphore_signal(
            barrier, inc=1, device_id=partner, device_id_type=pl.DeviceIdType.MESH
        )
    split = one.shape[0]
    acc[:split, :] = one[...]
    acc[split:, :] = two[...]
    pl.semaphore_wait(barrier, len(bits))
    size, start, used = acc.shape[0], 0, 0
    starts = []
    for step in range(len(bits)):
        half, place = size // 2, places[step]
        keep = pl.multiple_of(start + place * half, 16)
        give = pl.multiple_of(start + (1 - place) * half, 16)
        region = pl.ds(used, half)
        sent[region, :] = acc[pl.ds(give, half), :].astype(BF)
        copy = pltpu.make_async_remote_copy(
            src_ref=sent.at[region],
            dst_ref=got.at[region],
            send_sem=out_sem.at[step],
            recv_sem=in_sem.at[step],
            device_id=partners[step],
            device_id_type=pl.DeviceIdType.MESH,
        )
        copy.start()
        copy.wait()
        acc[pl.ds(keep, half), :] = acc[pl.ds(keep, half), :] + got[region, :].astype(F32)
        starts.append(keep)
        start, size, used = keep, half, used + half
    full[pl.ds(start, size), :] = acc[pl.ds(start, size), :].astype(BF)
    for step in reversed(range(len(bits))):
        region = pl.ds(starts[step], size)
        copy = pltpu.make_async_remote_copy(
            src_ref=full.at[region],
            dst_ref=full.at[region],
            send_sem=out_sem.at[len(bits) + step],
            recv_sem=in_sem.at[len(bits) + step],
            device_id=partners[step],
            device_id_type=pl.DeviceIdType.MESH,
        )
        copy.start()
        copy.wait()
        size = 2 * size
    one_out[...] = full[:split, :].astype(F32)
    two_out[...] = full[split:, :].astype(F32)


def total(one, two, sizes):
    bits = []
    for axis, count in (("mp", 2), *sizes):
        bit = 1 if (axis, count) == ("mp", 2) and not bits else (2 if axis == "mp" else 1)
        while bit < count:
            bits.append((axis, bit))
            bit *= 2
    rows, width = one.shape[0] + two.shape[0], one.shape[1]
    return pl.pallas_call(
        functools.partial(total_kernel, tuple(bits)),
        out_shape=(
            jax.ShapeDtypeStruct(one.shape, F32),
            jax.ShapeDtypeStruct(two.shape, F32),
        ),
        in_specs=[pl.BlockSpec(memory_space=pltpu.VMEM)] * 2,
        out_specs=(pl.BlockSpec(memory_space=pltpu.VMEM),) * 2,
        scratch_shapes=[
            pltpu.VMEM((rows, width), F32),
            pltpu.VMEM((rows, width), BF),
            pltpu.VMEM((rows, width), BF),
            pltpu.VMEM((rows, width), BF),
            pltpu.SemaphoreType.DMA((2 * len(bits),)),
            pltpu.SemaphoreType.DMA((2 * len(bits),)),
        ],
        compiler_params=pltpu.CompilerParams(
            collective_id=0, has_side_effects=True, vmem_limit_bytes=40 * 2**20
        ),
        name="total",
    )(one, two)


def spread_kernel(axis, count, one, out, out_sem, in_sem):
    mine = lax.axis_index(axis)
    barrier = pltpu.get_barrier_semaphore()
    others = [{axis: lax.rem(mine + by, count)} for by in range(1, count)]
    for other in others:
        pl.semaphore_signal(
            barrier, inc=1, device_id=other, device_id_type=pl.DeviceIdType.MESH
        )
    out[mine] = one[...]
    pl.semaphore_wait(barrier, count - 1)
    copies = []
    for i, other in enumerate(others):
        copy = pltpu.make_async_remote_copy(
            src_ref=one,
            dst_ref=out.at[mine],
            send_sem=out_sem.at[i],
            recv_sem=in_sem.at[i],
            device_id=other,
            device_id_type=pl.DeviceIdType.MESH,
        )
        copy.start()
        copies.append(copy)
    for copy in copies:
        copy.wait()


def spread(x, axis, count):
    return pl.pallas_call(
        functools.partial(spread_kernel, axis, count),
        out_shape=jax.ShapeDtypeStruct((count,) + x.shape, x.dtype),
        in_specs=[pl.BlockSpec(memory_space=pltpu.VMEM)],
        out_specs=pl.BlockSpec(memory_space=pltpu.VMEM),
        scratch_shapes=[
            pltpu.SemaphoreType.DMA((count - 1,)),
            pltpu.SemaphoreType.DMA((count - 1,)),
        ],
        compiler_params=pltpu.CompilerParams(collective_id=1, has_side_effects=True),
        name="spread",
    )(x)


def feed_kernel(
    count, own, cots, up_hbm, down_hbm, shift_ref, act_out, pre_out, grown_out, grad_out,
    two_out, up, down, near, cot, act, pre, grown, grad, load_sem, cot_sem, store_sem, out_sem, in_sem,
):
    mine = lax.axis_index("dp")
    tokens, width = own.shape
    hidden = up.shape[0]
    half, step = tokens // 2, 256
    order = by_bits(count)
    bits = [slot for slot in order if low_bit(slot) == slot]
    partner = {bit: {"dp": mine + (1 - 2 * ((mine // bit) % 2)) * bit} for bit in bits}
    barrier = pltpu.get_barrier_semaphore()
    for bit in bits:
        pl.semaphore_signal(
            barrier, inc=1, device_id=partner[bit], device_id_type=pl.DeviceIdType.MESH
        )
    weights = [
        pltpu.make_async_copy(up_hbm, up, load_sem.at[0]),
        pltpu.make_async_copy(down_hbm, down, load_sem.at[1]),
    ]
    for copy in weights:
        copy.start()

    def fetch(slot):
        return pltpu.make_async_copy(cots.at[slot], cot.at[slot % 2], cot_sem.at[slot % 2])

    def block(slot, which):
        rows = pl.ds(which * half, half)
        return own.at[rows] if slot == 0 else near.at[slot - 1, rows]

    def hop(slot, which):
        bit = (low_bit if which else high_bit)(slot)
        return pltpu.make_async_remote_copy(
            src_ref=block(slot ^ bit, which),
            dst_ref=block(slot, which),
            send_sem=out_sem.at[slot - 1, which],
            recv_sem=in_sem.at[slot - 1, which],
            device_id=partner[bit],
            device_id_type=pl.DeviceIdType.MESH,
        )

    hops = {(slot, which): hop(slot, which) for slot in order for which in range(2)}
    fetch(0).start()
    pl.semaphore_wait(barrier, len(bits))
    for bit in bits:
        for which in range(2):
            hops[bit, which].start()

    def stores(turn, slot):
        buf = turn % 2
        return [
            pltpu.make_async_copy(held.at[buf], out.at[slot], store_sem.at[buf, i])
            for i, (held, out) in enumerate(
                [(act, act_out), (pre, pre_out), (grown, grown_out), (grad, grad_out)]
            )
        ] + [
            pltpu.make_async_copy(
                own if slot == 0 else near.at[slot - 1], two_out.at[slot], store_sem.at[buf, 4]
            )
        ]

    sequence = [0] + order
    root = math.sqrt(2.0 / math.pi)

    def work(turn):
        slot, buf = sequence[turn], turn % 2
        if turn + 1 < count:
            following = sequence[turn + 1]
            pltpu.make_async_copy(
                cots.at[following], cot.at[1 - buf], cot_sem.at[1 - buf]
            ).start()
        pltpu.make_async_copy(cots.at[slot], cot.at[buf], cot_sem.at[buf]).wait()
        if turn == 0:
            for copy in weights:
                copy.wait()
        if turn >= 2:
            for copy in stores(turn - 2, sequence[turn - 2]):
                copy.wait()

        @pl.loop(0, hidden // step)
        def _(n):
            cols = pl.ds(pl.multiple_of(n * step, step), step)
            x = own[...] if slot == 0 else near[slot - 1]
            u = dot(x, up[cols, :], ((1,), (1,))) + shift_ref[:, cols]
            back = dot(cot[buf], down[cols, :], ((1,), (1,)))
            square = u * u
            bent = jnp.tanh(root * (u + 0.044715 * (square * u)))
            share = 0.5 * (1.0 + bent)
            slope = share + (0.5 * root) * u * (1.0 - bent * bent) * (1.0 + 0.134145 * square)
            act[buf, :, cols] = (u * share).astype(BF)
            pre[buf, :, cols] = (back * slope).astype(BF)

        @pl.loop(0, width // step)
        def _(n):
            cols = pl.ds(pl.multiple_of(n * step, step), step)
            grad[buf, :, cols] = dot(pre[buf], up[:, cols]).astype(BF)
            grown[buf, :, cols] = dot(act[buf], down[:, cols]).astype(BF)

        for copy in stores(turn, slot):
            copy.start()

    work(0)
    turn, place = 1, 0
    while place < len(order):
        level = [s for s in order if bin(s).count("1") == bin(order[place]).count("1")]
        for slot in level:
            for which in range(2):
                hops[slot, which].wait_recv()
            for later in order:
                for which in range(2):
                    bit = (low_bit if which else high_bit)(later)
                    if later ^ bit == slot:
                        hops[later, which].start()
        for slot in level:
            work(turn)
            turn += 1
        place += len(level)
    for key in hops:
        hops[key].wait_send()
    for turn in range(max(0, count - 2), count):
        for copy in stores(turn, sequence[turn]):
            copy.wait()


def feed_forward(own, cots, up, down, shift_row, count):
    tokens, width = own.shape
    hidden = up.shape[0]
    hbm = pl.BlockSpec(memory_space=pl.ANY)
    vmem = pl.BlockSpec(memory_space=pltpu.VMEM)
    slots = lambda columns: jax.ShapeDtypeStruct((count, tokens, columns), BF)
    return pl.pallas_call(
        functools.partial(feed_kernel, count),
        out_shape=(slots(hidden),) * 2 + (slots(width),) * 3,
        in_specs=[vmem, hbm, hbm, hbm, vmem],
        out_specs=(hbm,) * 5,
        scratch_shapes=[
            pltpu.VMEM((hidden, width), BF),
            pltpu.VMEM((hidden, width), BF),
            pltpu.VMEM((count - 1, tokens, width), BF),
            pltpu.VMEM((2, tokens, width), BF),
            pltpu.VMEM((2, tokens, hidden), BF),
            pltpu.VMEM((2, tokens, hidden), BF),
            pltpu.VMEM((2, tokens, width), BF),
            pltpu.VMEM((2, tokens, width), BF),
            pltpu.SemaphoreType.DMA((2,)),
            pltpu.SemaphoreType.DMA((2,)),
            pltpu.SemaphoreType.DMA((2, 5)),
            pltpu.SemaphoreType.DMA((count - 1, 2)),
            pltpu.SemaphoreType.DMA((count - 1, 2)),
        ],
        compiler_params=pltpu.CompilerParams(
            collective_id=2, has_side_effects=True, vmem_limit_bytes=60 * 2**20
        ),
        cost_estimate=pl.CostEstimate(
            flops=8 * count * tokens * width * hidden,
            bytes_accessed=16 * count * tokens * width,
            transcendentals=count * tokens * hidden,
        ),
        name="feed_forward",
    )(own, cots, up, down, shift_row)


def solution(mesh):
    ndp, nmp = mesh.shape["dp"], mesh.shape["mp"]

    def gather_mp(x):
        return lax.all_gather(x, "mp", axis=0, tiled=True)

    chips_of_core = [[core + 2 * chip for chip in range(nmp // 2)] for core in range(2)]

    def scatter_mp(x):
        return lax.psum_scatter(x, "mp", scatter_dimension=0, tiled=True)

    def body(
        block_input, segments, key_keep, ln1_gain, ln1_bias, w_query, b_query, w_keyval,
        b_value, w_out, b_out, ln2_gain, ln2_bias, w_up, b_up, w_down, b_down, cotangent,
    ):
        length, rows, width = block_input.shape
        tokens = length * rows
        hidden = w_up.shape[1]
        unit = hidden // ndp
        hidden_here = unit * nmp
        dp, mp = lax.axis_index("dp"), lax.axis_index("mp")

        def by_row(x):
            return jnp.swapaxes(x, 0, 1).reshape(tokens, width)

        def by_place(x):
            return jnp.swapaxes(x.reshape(rows, length, width), 0, 1)

        local = by_row(block_input)
        cot = by_row(cotangent)
        local_input = local.astype(F32)

        part = w_query.shape[1] // ndp
        chips = nmp // 2
        chip, core = mp // 2, mp % 2
        where = jnp.stack([dp, core]).astype(jnp.int32)
        full_length = segments.shape[1]
        reach = min(nmp - 1, -(-(full_length // 2 - 1) // length))

        normed = layer_norm(local_input, ln1_gain, ln1_bias).astype(BF)
        projected = dot(normed, w_keyval)
        keyval = jnp.concatenate(
            [projected[:, :HD], projected[:, HD:] + b_value], axis=1
        ).astype(BF).reshape(rows, length, 2 * HD)
        keyval = jnp.stack(
            [shift(keyval, "mp", nmp, by) for by in range(reach, 0, -1)] + [keyval]
        )

        def piece(shard, size):
            return lax.dynamic_slice_in_dim(shard, dp * size, size, 0)

        def gather_column(shard):
            return lax.all_gather(
                piece(shard, part), "mp", axis=0, tiled=True, axis_index_groups=chips_of_core
            )

        query_column = gather_column(w_query.T)
        out_column = gather_column(w_out)
        up_t = gather_mp(piece(w_up.T, unit))
        down = gather_mp(piece(w_down, unit))
        small_part = jnp.concatenate([b_query, piece(b_up, unit)])
        short = small_part.shape[0]
        small_part = jnp.pad(small_part, (0, -short % HD))
        biases = spread(small_part.reshape(-1, HD), "mp", nmp).reshape(nmp, -1)
        query_bias = biases[:, : b_query.shape[0]].reshape(-1)
        up_bias = biases[:, b_query.shape[0] : short].reshape(1, -1)

        def gather_heads(column):
            slots = gather_slots(column, "dp", ndp)
            return slots, [swap(slot, "mp", nmp, 1) for slot in slots]

        def weave_heads(near, far):
            slots = [slot.reshape(chips, part, width) for slot in near + far]
            return weave(slots, where, ndp).reshape(nmp * ndp * part, width)

        def sum_heads(*pairs):
            kinds = len(pairs)
            blocks = [
                jnp.concatenate([pair[slot].reshape(chips * part, width) for pair in pairs])
                for slot in range(ndp)
            ]
            column = scatter_slots(blocks, "dp", ndp).reshape(kinds, chips, part, width)
            blocks = [
                lax.dynamic_index_in_dim(column, chip ^ slot, 1, keepdims=False)
                .reshape(kinds * part, width)
                for slot in range(chips)
            ]
            slots = gather_slots(scatter_slots(blocks, "mp", nmp, 2), "dp", ndp)
            return [[slot[i * part : (i + 1) * part] for slot in slots] for i in range(kinds)]

        cot_near = gather_near(cot, "dp", ndp)
        near, far = gather_heads(query_column)
        bound = tie(out_column, *cot_near, *near, *far)
        out_column, cot_near = bound[0], bound[1 : 1 + len(cot_near)]
        near, far = bound[-2 * ndp : -ndp], bound[-ndp:]
        query_t = weave_heads(list(near), list(far))
        out_near, out_far = gather_heads(out_column)
        cot_slots = gather_far(cot, cot_near, "dp", ndp)

        window = (reach + 1) * length
        places = (mp - reach) * length + jnp.arange(window, dtype=jnp.int32)
        own_places = mp * length + jnp.arange(length, dtype=jnp.int32)

        def of_window(values):
            padded = jnp.pad(values, ((0, 0), (reach * length, 0)), constant_values=-1)
            return lax.dynamic_slice_in_dim(padded, mp * length, window, 1)

        own_segments = lax.dynamic_slice_in_dim(segments, mp * length, length, 1)
        same_place = places[None, :, None] == own_places[None, None, :]
        allowed = (
            (places[None, :, None] <= own_places[None, None, :])
            & (of_window(segments)[:, :, None] == own_segments[:, None, :])
            & ((of_window(key_keep)[:, :, None] == 1) | same_place)
        )
        bias = jnp.where(allowed, 0.0, NEG).astype(BF)
        bias = jnp.swapaxes(bias.reshape(rows, reach + 1, length, length), 0, 1)
        doc_start = jnp.sum((segments < own_segments[:, :1]).astype(jnp.int32), axis=1)
        span = jnp.maximum(doc_start // length - mp + reach, 0).astype(jnp.int32)

        queries = (dot(normed, query_t, ((1,), (1,))) + query_bias).astype(BF)
        attended, logs = attention_forward(span, queries, keyval, bias, rows)
        attended, *cot_slots = tie(attended, *cot_slots)
        out_full = weave_heads(out_near, out_far)
        residual = local_input + dot(attended, out_full) + b_out
        normed_two = layer_norm(residual, ln2_gain, ln2_bias).astype(BF)

        cot_full = jnp.stack(cot_slots)
        act_full, pre_full, grown, grad_two, two_full = feed_forward(
            normed_two, cot_full, up_t, down, up_bias, ndp
        )
        act_full, pre_full = act_full.reshape(-1, hidden_here), pre_full.reshape(-1, hidden_here)
        two_full = two_full.reshape(-1, width)
        with jax.named_scope("scatter_two"):
            grad_normed_two = scatter_slots(
                [grad_two[0].astype(F32)] + [grad_two[slot] for slot in range(1, ndp)], "dp", ndp
            )
        grad_down = dot(act_full, cot_full.reshape(-1, width), ((0,), (0,))).astype(BF)
        grad_up = dot(pre_full, two_full, ((0,), (0,))).astype(BF)
        grad_b_up = jnp.sum(pre_full, axis=0, dtype=F32)
        grad_normed_two, grad_up, grown = tie(grad_normed_two, grad_up, grown)
        grad_down, grad_up = scatter_mp(grad_down), scatter_mp(grad_up)

        norm_two_value, norm_two_pull = jax.vjp(layer_norm, residual, ln2_gain, ln2_bias)
        grad_resid_part, grad_ln2_gain, grad_ln2_bias = norm_two_pull(grad_normed_two)
        grad_residual = cot.astype(F32) + grad_resid_part
        grad_b_out = jnp.sum(grad_residual, axis=0)
        grad_b_down = jnp.sum(cot, axis=0, dtype=F32)
        grad_mixed = grad_residual.astype(BF)
        grad_attended = dot(grad_mixed, out_full, ((1,), (1,))).astype(BF)
        grad_attended, grad_down = tie(grad_attended, grad_down)
        down_near = gather_near(grad_down, "dp", ndp)
        theirs_out = pair_product(where, attended, grad_mixed, chips, ndp)
        theirs_out = swap(theirs_out, "mp", nmp, 1)
        steps = scatter_steps(
            [grown[0].astype(F32)] + [grown[slot] for slot in range(1, ndp)], "dp", ndp
        )
        values = next(steps)[1]
        for _ in range(ndp.bit_length() - 2):
            values = steps.send(steps.send(values)[1])[1]
        grad_attended, *values = tie(grad_attended, *values)
        values = steps.send(values)[1]
        grad_queries, grad_keyval = attention_backward(
            span, queries, grad_attended, attended, keyval, bias, logs, rows
        )
        mark = grad_keyval[0, 0, :16, :HD]

        def after_attention(values):
            return list(tie(mark, *values)[1:])

        theirs_query = pair_product(where, grad_queries, normed, chips, ndp)
        theirs_query = swap(theirs_query, "mp", nmp, 1)
        theirs_out, *down_near = after_attention([theirs_out, *down_near])
        down_slots = gather_far(grad_down, down_near, "dp", ndp)
        out_slots, query_slots = sum_heads(
            pair_product(where, attended, grad_mixed, chips, ndp, theirs_out),
            pair_product(where, grad_queries, normed, chips, ndp, theirs_query),
        )
        try:
            steps.send(after_attention(values))
        except StopIteration as end:
            grown_sum = end.value
        result = (residual + grown_sum + b_down).astype(BF)
        grad_keyval = sum(
            (
                shift(grad_keyval[reach - by], "mp", nmp, -by).astype(F32)
                for by in range(1, reach + 1)
            ),
            grad_keyval[reach].astype(F32),
        ).astype(BF).reshape(tokens, 2 * HD)
        grad_b_query = jnp.sum(grad_queries, axis=0, dtype=F32)
        grad_keyval, grad_up = tie(grad_keyval, grad_up)
        up_slots = gather_slots(grad_up, "dp", ndp)
        grad_normed = dot(grad_queries, query_t) + dot(grad_keyval, w_keyval, ((1,), (1,)))
        grad_w_keyval = dot(normed, grad_keyval, ((0,), (0,)))
        grad_b_value = jnp.sum(grad_keyval[:, HD:], axis=0, dtype=F32)
        norm_one_value, norm_one_pull = jax.vjp(layer_norm, local_input, ln1_gain, ln1_bias)
        grad_local, grad_ln1_gain, grad_ln1_bias = norm_one_pull(grad_normed)
        grad_input = (grad_residual + grad_local).astype(BF)

        units = jnp.zeros((nmp, ndp, unit), F32)
        units = lax.dynamic_update_slice(units, grad_b_up.reshape(nmp, 1, unit), (0, dp, 0))
        small = [
            grad_ln1_gain, grad_ln1_bias, grad_ln2_gain, grad_ln2_bias,
            grad_b_out, grad_b_down, grad_b_query, units.reshape(-1), grad_b_value,
        ]
        sizes = [value.shape[0] for value in small]
        cells = sum(sizes)
        lines = -(-cells // (2 * HD))
        lines += -(lines + width) % (16 * ndp * nmp)
        small.append(jnp.zeros((lines * 2 * HD - cells,), F32))
        small = jnp.concatenate(small).reshape(lines, 2 * HD)
        grad_w_keyval, sums = total(
            grad_w_keyval, small, (("dp", ndp), ("mp", nmp))
        )
        sums = sums.reshape(-1)
        pieces, place = [], 0
        for size in sizes:
            pieces.append(sums[place : place + size])
            place += size

        def own_part(value, size):
            return lax.dynamic_slice_in_dim(value, mp * size, size, 0)

        return (
            by_place(result),
            by_place(grad_input),
            pieces[0],
            pieces[1],
            settle(query_slots, where, True),
            own_part(pieces[6], b_query.shape[0]),
            grad_w_keyval,
            pieces[8],
            settle(out_slots, where, False),
            pieces[4],
            pieces[2],
            pieces[3],
            settle(up_slots, where, True),
            own_part(pieces[7], hidden),
            settle(down_slots, where, False),
            pieces[5],
        )

    return jax.shard_map(
        body,
        mesh=mesh,
        in_specs=(
            P("mp", "dp", None),
            P("dp", None),
            P("dp", None),
            P(),
            P(),
            P(None, "mp"),
            P("mp"),
            P(),
            P(),
            P("mp", None),
            P(),
            P(),
            P(),
            P(None, "mp"),
            P("mp"),
            P("mp", None),
            P(),
            P("mp", "dp", None),
        ),
        out_specs=(
            P("mp", "dp", None),
            P("mp", "dp", None),
            P(),
            P(),
            P(None, "mp"),
            P("mp"),
            P(),
            P(),
            P("mp", None),
            P(),
            P(),
            P(),
            P(None, "mp"),
            P("mp"),
            P("mp", None),
            P(),
        ),
        check_vma=False,
    )
```
